8 devices in a mesh: dp: 1 (over z), tp: 2 (over y), sp: 4 (over x, core).
Axes of the slice: x: 2, y: 2, z: 1, core: 2. Of those that a mesh axis runs over, the one named last changes fastest.
Arguments:
- features: bfloat16 [4, 256, 768], P('dp', 'sp')
- tokens: int32 [4, 512], P('dp', 'sp')
- lengths: int32 [4], P('dp')
- proj_w: bfloat16 [768, 2048], replicated
- proj_b: bfloat16 [2048], replicated
- embed: bfloat16 [256000, 2048], P('tp')
- ln_attn: bfloat16 [2, 2048], replicated
- w_query: bfloat16 [2, 2048, 2048], P(None, None, 'tp')
- w_key: bfloat16 [2, 2048, 256], replicated
- w_value: bfloat16 [2, 2048, 256], replicated
- w_out: bfloat16 [2, 2048, 2048], P(None, 'tp')
- ln_mlp: bfloat16 [2, 2048], replicated
- w_gate: bfloat16 [2, 2048, 16384], P(None, None, 'tp')
- w_up: bfloat16 [2, 2048, 16384], P(None, None, 'tp')
- w_down: bfloat16 [2, 16384, 2048], P(None, 'tp')
Outputs:
- output 1: bfloat16 [4, 256, 2048], P('dp', 'sp')
- output 2: bfloat16 [4, 512, 2048], P('dp', 'sp')
- output 3: bfloat16 [2, 2, 4, 256, 256], P(None, None, 'dp', 'sp')
- output 4: bfloat16 [2, 2, 4, 512, 256], P(None, None, 'dp', 'sp')
All inputs are finite; a program needn't handle non-finite values.
Results may differ from the reference program's by a relative error of at most 0.0141767.
Values are sent between devices in bfloat16 or wider.
A program may use at most 3 GiB of HBM per device.

```python
import jax
import jax.numpy as jnp
from jax import lax

BATCH_SIZE = 4
PROMPT_LEN = 512
IMAGE_TOKENS = 256
VISION_WIDTH = 768
MODEL_WIDTH = 2048
NUM_HEADS = 8
HEAD_DIM = 256
FF_WIDTH = 16384
VOCAB_SIZE = 256000
NUM_LAYERS = 2
DRAW_BLOCKS = 64
SEQ_LEN = IMAGE_TOKENS + PROMPT_LEN
NORM_EPS = 1e-6
ROPE_THETA = 10000.0


def draw_normal(rng_key, arr_shape, std_dev):
    return jax.random.normal(rng_key, arr_shape, jnp.float32) * std_dev


def setup_inputs(seed: int = 0, part: int = 0) -> dict:
    shared_keys = jax.random.split(jax.random.key(seed), 12)
    part_keys = jax.random.split(jax.random.fold_in(jax.random.key(seed + 1), part), 4)
    tokens = jax.random.randint(part_keys[1], (BATCH_SIZE, PROMPT_LEN), 0, VOCAB_SIZE, dtype=jnp.int32)
    drawn_lens = jax.random.randint(part_keys[2], (BATCH_SIZE,), PROMPT_LEN // 4 + 1, PROMPT_LEN + 1, dtype=jnp.int32)
    full_row = jax.random.randint(part_keys[3], (), 0, BATCH_SIZE, dtype=jnp.int32)
    lengths = jnp.where(jnp.arange(BATCH_SIZE) == full_row, PROMPT_LEN, drawn_lens).astype(jnp.int32)
    block_keys = jax.random.split(shared_keys[2], DRAW_BLOCKS)
    embed = lax.map(
        lambda blk_key: draw_normal(blk_key, (VOCAB_SIZE // DRAW_BLOCKS, MODEL_WIDTH), MODEL_WIDTH ** -0.5).astype(jnp.bfloat16),
        block_keys,
    ).reshape(VOCAB_SIZE, MODEL_WIDTH)
    qk_width = NUM_HEADS * HEAD_DIM
    return {
        "features": draw_normal(part_keys[0], (BATCH_SIZE, IMAGE_TOKENS, VISION_WIDTH), 1.0).astype(jnp.bfloat16),
        "tokens": tokens,
        "lengths": lengths,
        "proj_w": draw_normal(shared_keys[0], (VISION_WIDTH, MODEL_WIDTH), VISION_WIDTH ** -0.5).astype(jnp.bfloat16),
        "proj_b": draw_normal(shared_keys[1], (MODEL_WIDTH,), 0.5).astype(jnp.bfloat16),
        "embed": embed,
        "ln_attn": draw_normal(shared_keys[3], (NUM_LAYERS, MODEL_WIDTH), 0.3).astype(jnp.bfloat16),
        "w_query": draw_normal(shared_keys[4], (NUM_LAYERS, MODEL_WIDTH, qk_width), 1.5 * MODEL_WIDTH ** -0.5).astype(jnp.bfloat16),
        "w_key": draw_normal(shared_keys[5], (NUM_LAYERS, MODEL_WIDTH, HEAD_DIM), MODEL_WIDTH ** -0.5).astype(jnp.bfloat16),
        "w_value": draw_normal(shared_keys[6], (NUM_LAYERS, MODEL_WIDTH, HEAD_DIM), MODEL_WIDTH ** -0.5).astype(jnp.bfloat16),
        "w_out": draw_normal(shared_keys[7], (NUM_LAYERS, qk_width, MODEL_WIDTH), (SEQ_LEN / (16.0 * qk_width)) ** 0.5).astype(jnp.bfloat16),
        "ln_mlp": draw_normal(shared_keys[8], (NUM_LAYERS, MODEL_WIDTH), 0.3).astype(jnp.bfloat16),
        "w_gate": draw_normal(shared_keys[9], (NUM_LAYERS, MODEL_WIDTH, FF_WIDTH), MODEL_WIDTH ** -0.5).astype(jnp.bfloat16),
        "w_up": draw_normal(shared_keys[10], (NUM_LAYERS, MODEL_WIDTH, FF_WIDTH), MODEL_WIDTH ** -0.5).astype(jnp.bfloat16),
        "w_down": draw_normal(shared_keys[11], (NUM_LAYERS, FF_WIDTH, MODEL_WIDTH), FF_WIDTH ** -0.5).astype(jnp.bfloat16),
    }


def rms_norm(hidden, norm_gain):
    hid_f32 = hidden.astype(jnp.float32)
    mean_sq = jnp.mean(hid_f32 * hid_f32, axis=-1, keepdims=True)
    return (hid_f32 * lax.rsqrt(mean_sq + NORM_EPS) * (1.0 + norm_gain.astype(jnp.float32))).astype(jnp.bfloat16)


def rotary(vectors, cos_table, sin_table):
    half_dim = vectors.shape[-1] // 2
    first_half = vectors[..., :half_dim]
    second_half = vectors[..., half_dim:]
    return jnp.concatenate([first_half * cos_table - second_half * sin_table, second_half * cos_table + first_half * sin_table], axis=-1)


def reference(features, tokens, lengths, proj_w, proj_b, embed, ln_attn, w_query, w_key, w_value, w_out, ln_mlp, w_gate, w_up, w_down):
    half_dim = HEAD_DIM // 2
    inv_freq = ROPE_THETA ** (-jnp.arange(half_dim, dtype=jnp.float32) * (2.0 / HEAD_DIM))
    angles = jnp.arange(SEQ_LEN, dtype=jnp.float32)[:, None] * inv_freq[None, :]
    cos_table = jnp.cos(angles)
    sin_table = jnp.sin(angles)
    positions = jnp.arange(SEQ_LEN)
    emb_scale = MODEL_WIDTH ** 0.5
    layer_weights = (ln_attn, w_query, w_key, w_value, w_out, ln_mlp, w_gate, w_up, w_down)

    def one_request(request):
        feat_req, tok_req, len_req = request
        img_rows = (jnp.dot(feat_req, proj_w, preferred_element_type=jnp.float32) + proj_b.astype(jnp.float32)).astype(jnp.bfloat16)
        txt_rows = (jnp.take(embed, tok_req, axis=0).astype(jnp.float32) * emb_scale).astype(jnp.bfloat16)
        hidden_start = jnp.concatenate([img_rows, txt_rows], axis=0)
        key_valid = positions < IMAGE_TOKENS + len_req

        def layer_step(hidden, weights):
            gain_attn, wq_layer, wk_layer, wv_layer, wo_layer, gain_mlp, wg_layer, wu_layer, wd_layer = weights
            normed = rms_norm(hidden, gain_attn)
            queries = jnp.dot(normed, wq_layer, preferred_element_type=jnp.float32).reshape(SEQ_LEN, NUM_HEADS, HEAD_DIM)
            queries = rotary(queries, cos_table[:, None, :], sin_table[:, None, :]).astype(jnp.bfloat16)
            key_rows = rotary(jnp.dot(normed, wk_layer, preferred_element_type=jnp.float32), cos_table, sin_table).astype(jnp.bfloat16)
            value_rows = jnp.dot(normed, wv_layer, preferred_element_type=jnp.float32).astype(jnp.bfloat16)

            def attend_head(head_query):
                scores = jnp.dot(head_query, key_rows.T, preferred_element_type=jnp.float32) * HEAD_DIM ** -0.5
                scores = jnp.where(key_valid[None, :], scores, -1e30)
                attn_probs = jax.nn.softmax(scores, axis=-1).astype(jnp.bfloat16)
                return jnp.dot(attn_probs, value_rows, preferred_element_type=jnp.float32).astype(jnp.bfloat16)

            attn_heads = lax.map(attend_head, jnp.transpose(queries, (1, 0, 2)))
            attn_heads = jnp.transpose(attn_heads, (1, 0, 2)).reshape(SEQ_LEN, NUM_HEADS * HEAD_DIM)
            attn_out = jnp.dot(attn_heads, wo_layer, preferred_element_type=jnp.float32).astype(jnp.bfloat16)
            hidden = (hidden.astype(jnp.float32) + attn_out.astype(jnp.float32)).astype(jnp.bfloat16)
            normed = rms_norm(hidden, gain_mlp)
            gate_pre = jnp.dot(normed, wg_layer, preferred_element_type=jnp.float32)
            up_proj = jnp.dot(normed, wu_layer, preferred_element_type=jnp.float32)
            mlp_mix = (jax.nn.gelu(gate_pre, approximate=True) * up_proj).astype(jnp.bfloat16)
            down_out = jnp.dot(mlp_mix, wd_layer, preferred_element_type=jnp.float32).astype(jnp.bfloat16)
            hidden = (hidden.astype(jnp.float32) + down_out.astype(jnp.float32)).astype(jnp.bfloat16)
            return hidden, jnp.stack([key_rows, value_rows])

        return lax.scan(layer_step, hidden_start, layer_weights)

    hidden_all, cache_all = lax.map(one_request, (features, tokens, lengths))
    cache_all = jnp.transpose(cache_all, (1, 2, 0, 3, 4))
    return (hidden_all[:, :IMAGE_TOKENS], hidden_all[:, IMAGE_TOKENS:], cache_all[:, :, :, :IMAGE_TOKENS], cache_all[:, :, :, IMAGE_TOKENS:])
```

```python
import functools
import math
import jax
import jax.numpy as jnp
from jax import lax
from jax.experimental import pallas as pl
from jax.experimental.pallas import tpu as pltpu
from jax.sharding import PartitionSpec as P

NORM_EPS = 1e-6
ROPE_THETA = 10000.0
NUM_LAYERS = 2
F32 = jnp.float32
BF16 = jnp.bfloat16
MIB = 1024 * 1024
ANY = pl.BlockSpec(memory_space=pl.ANY)


def dot32(a, b):
    return jnp.dot(a, b, preferred_element_type=F32)


def rotate(vec, cos, sin):
    half = vec.shape[-1] // 2
    lo, hi = vec[:, :half], vec[:, half:]
    return jnp.concatenate([lo * cos - hi * sin, hi * cos + lo * sin], axis=-1)


def params(limit_mib, **kw):
    return pltpu.CompilerParams(vmem_limit_bytes=limit_mib * MIB, dimension_semantics=("arbitrary",), **kw)


def cost(flops, nbytes):
    return pl.CostEstimate(flops=int(flops), bytes_accessed=int(nbytes), transcendentals=0)


def kv_proj(layer, resid, parts, gain, w_key, w_value, cos, sin):
    reqs, seq, width = resid.shape
    hd = w_key.shape[2]

    def body(*refs):
        if parts:
            r_ref, p_ref, c0_ref, c1_ref, g_ref, wk_ref, wv_ref, cos_ref, sin_ref, h_ref, x_ref, kv_ref = refs
            got = jnp.concatenate([c0_ref[0], c1_ref[0]], axis=-1).astype(F32)
            mlp = (p_ref[0].astype(F32) + got).astype(BF16)
            hid = (r_ref[0].astype(F32) + mlp.astype(F32)).astype(BF16)
            h_ref[0] = hid
        else:
            r_ref, g_ref, wk_ref, wv_ref, cos_ref, sin_ref, x_ref, kv_ref = refs
            hid = r_ref[0]
        hid = hid.astype(F32)
        ms = jnp.mean(hid * hid, axis=-1, keepdims=True)
        x = (hid * lax.rsqrt(ms + NORM_EPS) * (1.0 + g_ref[layer:layer + 1, :].astype(F32))).astype(BF16)
        x_ref[0] = x
        kv_ref[0, 0] = rotate(dot32(x, wk_ref[0]), cos_ref[...], sin_ref[...]).astype(BF16)
        kv_ref[1, 0] = dot32(x, wv_ref[0]).astype(BF16)

    row = pl.BlockSpec((1, seq, width), lambda i: (i, 0, 0))
    halfrow = pl.BlockSpec((1, seq, width // 2), lambda i: (i, 0, 0))
    wspec = pl.BlockSpec((1, width, hd), lambda i: (layer, 0, 0))
    rope = pl.BlockSpec((seq, hd // 2), lambda i: (0, 0))
    gspec = pl.BlockSpec(gain.shape, lambda i: (0, 0))
    rows = jax.ShapeDtypeStruct((reqs, seq, width), BF16)
    kv_shape = jax.ShapeDtypeStruct((2, reqs, seq, hd), BF16)
    kv_spec = pl.BlockSpec((2, 1, seq, hd), lambda i: (0, i, 0, 0))
    ins, in_specs = [resid], [row]
    outs, out_specs = [rows, kv_shape], [row, kv_spec]
    if parts:
        ins += list(parts)
        in_specs += [row, halfrow, halfrow]
        outs, out_specs = [rows] + outs, [row] + out_specs
    res = pl.pallas_call(
        body, grid=(reqs,), out_shape=outs, in_specs=in_specs + [gspec, wspec, wspec, rope, rope], out_specs=out_specs,
        compiler_params=params(48), name=f"kv_proj{layer}",
        cost_estimate=cost(4 * reqs * seq * width * hd, 8 * MIB),
    )(*ins, gain, w_key, w_value, cos, sin)
    return res if parts else [resid] + list(res)


def attend(layer, x, weights, local, kvs, mask, cos, sin):
    reqs, seq, width = x.shape
    hd = kvs[0].shape[3]
    heads = 4
    keys = len(kvs) * seq
    expo = hd ** -0.5 * math.log2(math.e)
    nw = len(weights)

    def body(*refs):
        x_ref, mask_ref, cos_ref, sin_ref = refs[:4]
        w_refs = refs[4:4 + nw]
        kv_refs = refs[4 + nw:4 + nw + len(kvs)]
        o_ref, wbuf, kvbuf, wsem, kvsem = refs[4 + nw + len(kvs):]
        head = pl.program_id(0)

        def w_copy(i):
            src = w_refs[0].at[layer, :, pl.ds(i * hd, hd)] if local else w_refs[i]
            return pltpu.make_async_copy(src, wbuf.at[i], wsem.at[i])

        def kv_copy(i):
            return pltpu.make_async_copy(kv_refs[i], kvbuf.at[:, :, pl.ds(i * seq, seq), :], kvsem.at[i])

        @pl.when(head == 0)
        def _():
            w_copy(0).start()
            for i in range(len(kvs)):
                kv_copy(i).start()
            for i in range(1, heads):
                w_copy(i).start()

        for i in range(heads):
            @pl.when(head == i)
            def _(i=i):
                w_copy(i).wait()

        q = dot32(x_ref[...].reshape(reqs * seq, width), wbuf[head])

        @pl.when(head == 0)
        def _():
            for i in range(len(kvs)):
                kv_copy(i).wait()

        for r in range(reqs):
            qr = rotate(q[r * seq:(r + 1) * seq], cos_ref[...], sin_ref[...]).astype(BF16)
            s = lax.dot_general(qr, kvbuf[0, r], (((1,), (1,)), ((), ())), preferred_element_type=F32)
            s = jnp.where(mask_ref[r:r + 1, :] > 0, s, -1e30)
            top = jnp.max(s, axis=-1, keepdims=True)
            p = jnp.exp2((s - top) * expo)
            p = (p * (1.0 / jnp.sum(p, axis=-1, keepdims=True))).astype(BF16)
            o_ref[r] = dot32(p, kvbuf[1, r]).astype(BF16)

    full = lambda a: pl.BlockSpec(a.shape, lambda i: (0,) * a.ndim)
    return pl.pallas_call(
        body, grid=(heads,), out_shape=jax.ShapeDtypeStruct((reqs, seq, heads * hd), BF16),
        in_specs=[full(x), full(mask), full(cos), full(sin)] + [ANY] * (nw + len(kvs)),
        out_specs=pl.BlockSpec((reqs, seq, hd), lambda i: (0, 0, i)),
        scratch_shapes=[pltpu.VMEM((heads, width, hd), BF16), pltpu.VMEM((2, reqs, keys, hd), BF16),
                        pltpu.SemaphoreType.DMA((heads,)), pltpu.SemaphoreType.DMA((len(kvs),))],
        compiler_params=params(48), name=f"attend{layer}_{'loc' if local else 'rem'}",
        cost_estimate=cost(2 * reqs * seq * heads * hd * (width + 2 * keys), 8 * MIB),
    )(x, mask, cos, sin, *weights, *kvs)


def out_proj(layer, o_loc, o_rem, hid, w_out, pieces, gain):
    reqs, seq, half = o_loc.shape
    width = hid.shape[2]
    rows = reqs * seq
    bn = 256
    steps = width // bn
    hd = pieces[0].shape[0]

    def body(ol_ref, or_ref, h_ref, g_ref, w_ref, *refs):
        p_refs = refs[:len(pieces)]
        h1_ref, x_ref, wbuf, ssq, sem = refs[len(pieces):]
        step = pl.program_id(0)

        def copies(n):
            cols = pl.ds(n * bn, bn)
            out = [pltpu.make_async_copy(w_ref.at[layer, :, cols], wbuf.at[n, pl.ds(0, half), :], sem.at[n, 0])]
            for i, p in enumerate(p_refs):
                out.append(pltpu.make_async_copy(p.at[:, cols], wbuf.at[n, pl.ds(half + i * hd, hd), :], sem.at[n, 1 + i]))
            return out

        @pl.when(step == 0)
        def _():
            for n in range(steps):
                for c in copies(n):
                    c.start()
            ssq[...] = jnp.zeros_like(ssq)

        for c in copies(step):
            c.wait()
        w = wbuf[step]
        acc = dot32(ol_ref[...].reshape(rows, half), w[:half]) + dot32(or_ref[...].reshape(rows, half), w[half:])
        h1 = (h_ref[...].reshape(rows, bn).astype(F32) + acc.astype(BF16).astype(F32)).astype(BF16)
        h1_ref[:, :, pl.ds(pl.multiple_of(step * bn, bn), bn)] = h1.reshape(reqs, seq, bn)
        h1 = h1.astype(F32)
        sq = h1 * h1
        ssq[...] += sum(sq[:, j:j + 128] for j in range(0, bn, 128))

        @pl.when(step == steps - 1)
        def _():
            ms = jnp.sum(ssq[...], axis=-1, keepdims=True) * (1.0 / width)
            full = h1_ref[...].reshape(rows, width).astype(F32)
            x = full * lax.rsqrt(ms + NORM_EPS) * (1.0 + g_ref[layer:layer + 1, :].astype(F32))
            x_ref[...] = x.astype(BF16).reshape(reqs, seq, width)

    full = lambda a: pl.BlockSpec(a.shape, lambda i: (0,) * a.ndim)
    shape = jax.ShapeDtypeStruct(hid.shape, BF16)
    return pl.pallas_call(
        body, grid=(steps,), out_shape=[shape, shape],
        in_specs=[full(o_loc), full(o_rem), pl.BlockSpec((reqs, seq, bn), lambda i: (0, 0, i)), full(gain), ANY] + [ANY] * len(pieces),
        out_specs=[full(hid), full(hid)],
        scratch_shapes=[pltpu.VMEM((steps, width, bn), BF16), pltpu.VMEM((rows, 128), F32),
                        pltpu.SemaphoreType.DMA((steps, 1 + len(pieces)))],
        compiler_params=params(48), name=f"out_proj{layer}",
        cost_estimate=cost(2 * rows * width * width, 12 * MIB),
    )(o_loc, o_rem, hid, gain, w_out, *pieces)


def gate_up(layer, x, w_gate, w_up, tag):
    rows, width = x.shape
    ff = w_gate.shape[2]
    bn = 512
    sub = 256

    def body(x_ref, g_ref, u_ref, a_ref):
        for j in range(bn // sub):
            cols = slice(j * sub, (j + 1) * sub)
            gate = dot32(x_ref[...], g_ref[0, :, cols])
            up = dot32(x_ref[...], u_ref[0, :, cols])
            a_ref[:, cols] = (jax.nn.gelu(gate, approximate=True) * up).astype(BF16)

    wspec = pl.BlockSpec((1, width, bn), lambda i: (layer, 0, i))
    return pl.pallas_call(
        body, grid=(ff // bn,), out_shape=jax.ShapeDtypeStruct((rows, ff), BF16),
        in_specs=[pl.BlockSpec((rows, width), lambda i: (0, 0)), wspec, wspec],
        out_specs=pl.BlockSpec((rows, bn), lambda i: (0, i)),
        compiler_params=params(48), name=f"gate_up{layer}_{tag}",
        cost_estimate=cost(4 * rows * width * ff, 4 * width * ff),
    )(x, w_gate, w_up)


def down(layer, a, w_down, first, count, tag):
    rows, ff = a.shape
    bn = 256

    def body(a_ref, w_ref, o_ref):
        o_ref[...] = dot32(a_ref[...], w_ref[0]).astype(BF16)

    return pl.pallas_call(
        body, grid=(count // bn,), out_shape=jax.ShapeDtypeStruct((rows, count), BF16),
        in_specs=[pl.BlockSpec((rows, ff), lambda i: (0, 0)), pl.BlockSpec((1, ff, bn), lambda i: (layer, 0, first // bn + i))],
        out_specs=pl.BlockSpec((rows, bn), lambda i: (0, i)),
        compiler_params=params(48), name=f"down{layer}_{tag}",
        cost_estimate=cost(2 * rows * ff * count, 2 * ff * count),
    )(a, w_down)


def after(value, *deps):
    return lax.optimization_barrier((value,) + deps)[0]


def solution(mesh):
    sp_size = mesh.shape["sp"]
    tp_size = mesh.shape["tp"]
    in_specs = (P("dp", "sp", None), P("dp", "sp"), P("dp"), P(), P(), P("tp", None), P(), P(None, None, "tp"), P(), P(), P(None, "tp", None), P(), P(None, None, "tp"), P(None, None, "tp"), P(None, "tp", None))
    out_specs = (P("dp", "sp", None), P("dp", "sp", None), P(None, None, "dp", "sp", None), P(None, None, "dp", "sp", None))
    swap = lambda v: lax.ppermute(v, "tp", [(i, tp_size - 1 - i) for i in range(tp_size)])
    hop = lambda v, bit: lax.ppermute(v, "sp", [(i, i ^ bit) for i in range(sp_size)])

    def device_fn(features, tokens, lengths, proj_w, proj_b, embed, ln_attn, w_query, w_key, w_value, w_out, ln_mlp, w_gate, w_up, w_down):
        num_req, img_loc, _ = features.shape
        txt_loc = tokens.shape[1]
        seq = img_loc + txt_loc
        width = proj_w.shape[1]
        hd = w_key.shape[2]
        rows_loc = embed.shape[0]
        sp = lax.axis_index("sp")
        tp = lax.axis_index("tp")
        half = num_req // tp_size
        mine = lambda v, axis=0: lax.dynamic_slice_in_dim(v, tp * half, half, axis)
        theirs = lambda v, axis=0: lax.dynamic_slice_in_dim(v, (tp_size - 1 - tp) * half, half, axis)

        def query_piece(layer):
            return lax.dynamic_slice(w_query, (layer, 0, sp * hd), (1, width, hd))[0]

        def out_piece(layer):
            return lax.dynamic_slice(w_out, (layer, sp * hd, 0), (1, hd, width))[0]

        def spread(piece):
            mate = hop(piece, 1)
            far = hop(piece, 2)
            return [piece, mate, far, hop(far, 1)]

        def rows_of(ids):
            return jnp.take(embed, jnp.clip(ids - tp * rows_loc, 0, rows_loc - 1).reshape(-1), axis=0, mode="clip")

        wq_pieces = [spread(swap(query_piece(0))), None]
        their_rows = rows_of(theirs(tokens))
        got_rows = swap(their_rows)
        my_ids = mine(tokens)
        my_rows = rows_of(after(my_ids, their_rows))
        owned = (my_ids >= tp * rows_loc) & (my_ids < (tp + 1) * rows_loc)
        img = (jnp.einsum("bpc,cd->bpd", mine(features), proj_w, preferred_element_type=F32) + proj_b.astype(F32)).astype(BF16)
        picked = jnp.where(owned.reshape(-1)[:, None], my_rows, got_rows)
        txt = (picked.astype(F32) * math.sqrt(width)).astype(BF16).reshape(half, txt_loc, width)
        hidden = jnp.concatenate([img, txt], axis=1)
        wo_pieces = [spread(swap(after(out_piece(0), got_rows))), None]

        positions = jnp.concatenate([sp * img_loc + jnp.arange(img_loc), img_loc * sp_size + sp * txt_loc + jnp.arange(txt_loc)])
        inv_freq = ROPE_THETA ** (-jnp.arange(hd // 2, dtype=F32) * (2.0 / hd))
        angles = positions.astype(F32)[:, None] * inv_freq[None, :]
        cos, sin = jnp.cos(angles), jnp.sin(angles)
        slot = jnp.arange(seq)[None, :]
        owner = jnp.stack([sp ^ b for b in range(sp_size)])[:, None]
        text_index = (owner * txt_loc + slot - img_loc).reshape(1, -1)
        is_img = jnp.broadcast_to(slot < img_loc, (sp_size, seq)).reshape(1, -1)
        mask = (is_img | (text_index < mine(lengths)[:, None])).astype(F32)

        parts = ()
        caches = []
        for layer in range(NUM_LAYERS):
            hidden, x, kv = kv_proj(layer, hidden, parts, ln_attn, w_key, w_value, cos, sin)
            far = hop(kv, 2)
            kvs = [kv, hop(kv, 1), far, hop(far, 1)]
            caches.append((kv, swap(kv)))
            o_loc = attend(layer, x, [w_query], True, kvs, mask, cos, sin)
            o_rem = attend(layer, x, wq_pieces[layer], False, kvs, mask, cos, sin)
            if layer + 1 == NUM_LAYERS:
                o_loc = after(o_loc, *[c for _, c in caches])
            h1, x2 = out_proj(layer, o_loc, o_rem, hidden, w_out, wo_pieces[layer], ln_mlp)
            x2 = x2.reshape(half * seq, width)
            x2p = swap(x2)
            if layer + 1 < NUM_LAYERS:
                wq_pieces[layer + 1] = spread(swap(after(query_piece(layer + 1), x2p)))
                wo_pieces[layer + 1] = spread(swap(after(out_piece(layer + 1), x2p)))
            a_mine = gate_up(layer, x2, w_gate, w_up, "own")
            a_their = gate_up(layer, x2p, w_gate, w_up, "oth")
            back = [swap(down(layer, a_their, w_down, i * width // 2, width // 2, f"oth{i}")) for i in range(2)]
            own = down(layer, a_mine, w_down, 0, width, "own")
            shape = (half, seq, -1)
            parts = (own.reshape(shape), back[0].reshape(shape), back[1].reshape(shape))
            hidden = h1
        mlp = (parts[0].astype(F32) + jnp.concatenate(parts[1:], axis=-1).astype(F32)).astype(BF16)
        hidden = (hidden.astype(F32) + mlp.astype(F32)).astype(BF16)
        other = swap(hidden)

        def merge(a, b, axis):
            return jnp.where(tp == 0, jnp.concatenate([a, b], axis), jnp.concatenate([b, a], axis))

        cache = jnp.stack([merge(a, b, 1) for a, b in caches])
        final = merge(hidden, other, 0)
        return final[:, :img_loc], final[:, img_loc:], cache[:, :, :, :img_loc], cache[:, :, :, img_loc:]

    return jax.shard_map(device_fn, mesh=mesh, in_specs=in_specs, out_specs=out_specs, check_vma=False)
```

```python
import functools
import math
import jax
import jax.numpy as jnp
from jax import lax
from jax.experimental import pallas as pl
from jax.experimental.pallas import tpu as pltpu
from jax.sharding import PartitionSpec as P

NORM_EPS = 1e-6
ROPE_THETA = 10000.0
NUM_LAYERS = 2
F32 = jnp.float32
BF16 = jnp.bfloat16
MIB = 1024 * 1024
ANY = pl.BlockSpec(memory_space=pl.ANY)


def dot32(a, b):
    return jnp.dot(a, b, preferred_element_type=F32)


def rotate(vec, cos, sin):
    half = vec.shape[-1] // 2
    lo, hi = vec[:, :half], vec[:, half:]
    return jnp.concatenate([lo * cos - hi * sin, hi * cos + lo * sin], axis=-1)


def params(limit_mib, **kw):
    return pltpu.CompilerParams(vmem_limit_bytes=limit_mib * MIB, dimension_semantics=("arbitrary",), **kw)


def cost(flops, nbytes):
    return pl.CostEstimate(flops=int(flops), bytes_accessed=int(nbytes), transcendentals=0)


def full(a):
    return pl.BlockSpec(a.shape, lambda *i: (0,) * a.ndim)


def normed(hid, gain):
    hid = hid.astype(F32)
    ms = jnp.mean(hid * hid, axis=-1, keepdims=True)
    return (hid * lax.rsqrt(ms + NORM_EPS) * (1.0 + gain.astype(F32))).astype(BF16)


def kv_proj(layer, hid, gain, w_key, w_value, cos, sin, tag):
    reqs, seq, width = hid.shape
    hd = w_key.shape[2]

    def body(h_ref, g_ref, wk_ref, wv_ref, cos_ref, sin_ref, x_ref, kv_ref):
        x = normed(h_ref[0], g_ref[layer:layer + 1, :])
        x_ref[0] = x
        kv_ref[0, 0] = rotate(dot32(x, wk_ref[0]), cos_ref[...], sin_ref[...]).astype(BF16)
        kv_ref[1, 0] = dot32(x, wv_ref[0]).astype(BF16)

    row = pl.BlockSpec((1, seq, width), lambda i: (i, 0, 0))
    wspec = pl.BlockSpec((1, width, hd), lambda i: (layer, 0, 0))
    return pl.pallas_call(
        body, grid=(reqs,),
        out_shape=[jax.ShapeDtypeStruct(hid.shape, BF16), jax.ShapeDtypeStruct((2, reqs, seq, hd), BF16)],
        in_specs=[row, full(gain), wspec, wspec, full(cos), full(sin)],
        out_specs=[row, pl.BlockSpec((2, 1, seq, hd), lambda i: (0, i, 0, 0))],
        compiler_params=params(58), name=f"kv_proj{layer}{tag}",
        cost_estimate=cost(4 * reqs * seq * width * hd, 6 * MIB),
    )(hid, gain, w_key, w_value, cos, sin)


def q_proj(layer, x, w_query, pieces, cos, sin, tag):
    reqs, seq, width = x.shape
    hd = 2 * cos.shape[1]
    local = w_query.shape[2] // hd
    heads = local + (local if pieces is not None else 0)

    def body(x_ref, cos_ref, sin_ref, w_ref, *refs):
        q_ref, wbuf, sem = refs[-3:]
        head = pl.program_id(0)

        def copy(i):
            src = w_ref.at[layer, :, pl.ds(i * hd, hd)] if i < local else refs[0].at[i - local]
            return pltpu.make_async_copy(src, wbuf.at[i], sem.at[i])

        @pl.when(head == 0)
        def _():
            for i in range(heads):
                copy(i).start()

        for i in range(heads):
            @pl.when(head == i)
            def _(i=i):
                copy(i).wait()

        q = dot32(x_ref[...].reshape(reqs * seq, width), wbuf[head])
        for r in range(reqs):
            q_ref[r, 0] = rotate(q[r * seq:(r + 1) * seq], cos_ref[...], sin_ref[...]).astype(BF16)

    extra = [] if pieces is None else [pieces]
    return pl.pallas_call(
        body, grid=(heads,), out_shape=jax.ShapeDtypeStruct((reqs, heads, seq, hd), BF16),
        in_specs=[full(x), full(cos), full(sin), ANY] + [ANY] * len(extra),
        out_specs=pl.BlockSpec((reqs, 1, seq, hd), lambda i: (0, i, 0, 0)),
        scratch_shapes=[pltpu.VMEM((heads, width, hd), BF16), pltpu.SemaphoreType.DMA((heads,))],
        compiler_params=params(58), name=f"q_proj{layer}{tag}",
        cost_estimate=cost(2 * reqs * seq * heads * hd * width, 2 * heads * hd * width),
    )(x, cos, sin, w_query, *extra)


def attend(layer, q, kvs, mask, tag):
    reqs, heads, seq, hd = q.shape
    keys = len(kvs) * seq
    expo = hd ** -0.5 * math.log2(math.e)
    pair = 2

    def body(q_ref, mask_ref, *refs):
        o_ref = refs[-1]
        k = jnp.concatenate([ref[0, 0] for ref in refs[:-1]], axis=0)
        v = jnp.concatenate([ref[1, 0] for ref in refs[:-1]], axis=0)
        valid = mask_ref[0] > 0
        for j in range(pair):
            s = lax.dot_general(q_ref[0, j], k, (((1,), (1,)), ((), ())), preferred_element_type=F32)
            s = jnp.where(valid, s, -1e30)
            top = jnp.max(s, axis=-1, keepdims=True)
            p = jnp.exp2((s - top) * expo)
            p = (p * (1.0 / jnp.sum(p, axis=-1, keepdims=True))).astype(BF16)
            o_ref[0, :, j * hd:(j + 1) * hd] = dot32(p, v).astype(BF16)

    kvspec = pl.BlockSpec((2, 1, seq, hd), lambda r, g: (0, r, 0, 0))
    return pl.pallas_call(
        body, grid=(reqs, heads // pair), out_shape=jax.ShapeDtypeStruct((reqs, seq, heads * hd), BF16),
        in_specs=[pl.BlockSpec((1, pair, seq, hd), lambda r, g: (r, g, 0, 0)), pl.BlockSpec((1, 1, keys), lambda r, g: (r, 0, 0))] + [kvspec] * len(kvs),
        out_specs=pl.BlockSpec((1, seq, pair * hd), lambda r, g: (r, 0, g)),
        compiler_params=pltpu.CompilerParams(vmem_limit_bytes=24 * MIB, dimension_semantics=("arbitrary", "arbitrary")), name=f"attend{layer}{tag}",
        cost_estimate=cost(4 * reqs * seq * heads * hd * keys, 6 * MIB),
    )(q, mask, *kvs)


def out_proj(layer, o, w_out, pieces, hid, back, tag):
    reqs, seq, depth = o.shape
    width = w_out.shape[2]
    half = w_out.shape[1]
    rows = reqs * seq
    bn = 256
    steps = width // bn
    extra = [] if pieces is None else [pieces]
    adds = [a for a in (hid, back) if a is not None]

    def body(o_ref, w_ref, *refs):
        p_ref = refs[0] if extra else None
        add_refs = refs[len(extra):len(extra) + len(adds)]
        y_ref, wbuf, sem = refs[-3:]
        step = pl.program_id(0)

        def copies(n):
            cols = pl.ds(pl.multiple_of(n * bn, bn), bn)
            out = [pltpu.make_async_copy(w_ref.at[layer, :, cols], wbuf.at[n, pl.ds(0, half), :], sem.at[n, 0])]
            if extra:
                hd = pieces.shape[1]
                for i in range(pieces.shape[0]):
                    out.append(pltpu.make_async_copy(p_ref.at[i, :, cols], wbuf.at[n, pl.ds(half + i * hd, hd), :], sem.at[n, 1 + i]))
            return out

        @pl.when(step == 0)
        def _():
            for n in range(steps):
                for c in copies(n):
                    c.start()

        for c in copies(step):
            c.wait()
        acc = dot32(o_ref[...].reshape(rows, depth), wbuf[step])
        if back is not None:
            acc = acc + add_refs[1][...].reshape(rows, bn).astype(F32)
        acc = acc.astype(BF16)
        if hid is not None:
            acc = (add_refs[0][...].reshape(rows, bn).astype(F32) + acc.astype(F32)).astype(BF16)
        y_ref[...] = acc.reshape(reqs, seq, bn)

    col = pl.BlockSpec((reqs, seq, bn), lambda i: (0, 0, i))
    return pl.pallas_call(
        body, grid=(steps,), out_shape=jax.ShapeDtypeStruct((reqs, seq, width), BF16),
        in_specs=[full(o), ANY] + [ANY] * len(extra) + [col] * len(adds), out_specs=col,
        scratch_shapes=[pltpu.VMEM((steps, depth, bn), BF16), pltpu.SemaphoreType.DMA((steps, 5))],
        compiler_params=params(58), name=f"out_proj{layer}{tag}",
        cost_estimate=cost(2 * rows * depth * width, 2 * depth * width),
    )(o, w_out, *extra, *adds)


def mlp(layer, last, h1, gain, w_gate, w_up, w_down, w_query, w_out):
    rows, width = h1.shape
    ff = w_gate.shape[2]
    bn = 1024
    sub = 256
    gu_steps = ff // bn
    dn = 256
    dn_steps = width // dn
    gu_slots, dn_slots = 2, 3
    norm_rows = 48
    hd = 256

    def body(h_ref, g_ref, wg_ref, wu_ref, wd_ref, wq_ref, wo_ref, *refs):
        if last:
            out_ref, hoth, x, a, gub, dnb, sent, got, gsem, dsem, hsem, ssem, rsem = refs
        else:
            out_ref, wqn, won, hoth, x, a, gub, dnb, sent, got, gsem, dsem, hsem, ssem, rsem, wsem = refs
        tp = lax.axis_index("tp")
        sp = lax.axis_index("sp")
        other = {"tp": 1 - tp}
        mate = {"sp": sp + 1 - 2 * lax.rem(sp, 2)}
        far = {"sp": lax.rem(sp + 2, 4)}
        peers = [other] if last else [other, mate, far]
        send = functools.partial(pltpu.make_async_remote_copy, device_id_type=pl.DeviceIdType.MESH)

        def gu_copies(i, slot):
            cols = pl.ds(pl.multiple_of(lax.rem(i, gu_steps) * bn, bn), bn)
            return [pltpu.make_async_copy(w.at[layer, :, cols], gub.at[slot, k], gsem.at[slot, k]) for k, w in enumerate((wg_ref, wu_ref))]

        def dn_copy(i, slot):
            cols = pl.ds(pl.multiple_of(lax.rem(i, dn_steps) * dn, dn), dn)
            return pltpu.make_async_copy(wd_ref.at[layer, :, cols], dnb.at[slot], dsem.at[slot])

        for i in range(gu_slots):
            for c in gu_copies(i, i):
                c.start()
        for i in range(dn_slots):
            dn_copy(i, i).start()
        barrier = pltpu.get_barrier_semaphore()
        for peer in peers:
            pl.semaphore_signal(barrier, inc=1, device_id=peer, device_id_type=pl.DeviceIdType.MESH)
        pl.semaphore_wait(barrier, len(peers))
        h_copy = send(src_ref=h_ref, dst_ref=hoth, send_sem=hsem.at[0], recv_sem=hsem.at[1], device_id=other)
        h_copy.start()

        def norm(src):
            def step(i, _):
                r = pl.ds(pl.multiple_of(i * norm_rows, norm_rows), norm_rows)
                x[r, :] = normed(src[r, :], g_ref[layer:layer + 1, :])
                return 0
            lax.fori_loop(0, rows // norm_rows, step, 0)

        def gate_up(first, total, side):
            def step(c, _):
                i = first + c
                slot = lax.rem(i, gu_slots)
                for cp in gu_copies(i, slot):
                    cp.wait()
                for j in range(bn // sub):
                    cols = slice(j * sub, (j + 1) * sub)
                    gate = dot32(x[...], gub[slot, 0, :, cols])
                    up = dot32(x[...], gub[slot, 1, :, cols])
                    mix = (jax.nn.gelu(gate, approximate=True) * up).astype(BF16)
                    a[side, :, pl.ds(pl.multiple_of(c * bn + j * sub, sub), sub)] = mix

                @pl.when(i + gu_slots < total)
                def _():
                    for cp in gu_copies(i + gu_slots, slot):
                        cp.start()
                return 0
            lax.fori_loop(0, gu_steps, step, 0)

        def part_copy(k, n):
            return send(src_ref=sent.at[k, n], dst_ref=got.at[k, n], send_sem=ssem.at[k, n], recv_sem=rsem.at[k, n], device_id=other)

        def cols_of(n):
            return pl.ds(pl.multiple_of(n * dn, dn), dn)

        norm(h_ref)
        gate_up(0, 2 * gu_steps, 0)
        if last:
            def own_step(n, _):
                slot = lax.rem(n, dn_slots)
                dn_copy(n, slot).wait()
                sent[0, n] = dot32(a[0], dnb[slot]).astype(BF16)

                @pl.when(n > 0)
                def _():
                    part_copy(0, n - 1).start()
                dn_copy(n + dn_slots, slot).start()
                return 0
            lax.fori_loop(0, dn_steps, own_step, 0)
            h_copy.wait()
            norm(hoth)
            part_copy(0, dn_steps - 1).start()
            gate_up(gu_steps, 2 * gu_steps, 0)
            reqs = out_ref.shape[0] // 2
            seq = out_ref.shape[1]

            def write(first, src, k, n):
                mix = (sent[1 - k, n].astype(F32) + got[k, n].astype(F32)).astype(BF16)
                y = (src[:, cols_of(n)].astype(F32) + mix.astype(F32)).astype(BF16)
                out_ref[pl.ds(first * reqs, reqs), :, cols_of(n)] = y.reshape(reqs, seq, dn)

            def oth_step(n, _):
                i = dn_steps + n
                slot = lax.rem(i, dn_slots)
                dn_copy(i, slot).wait()
                sent[1, n] = dot32(a[0], dnb[slot]).astype(BF16)
                part_copy(0, n).wait()
                write(1 - tp, hoth, 0, n)
                part_copy(1, n).start()

                @pl.when(i + dn_slots < 2 * dn_steps)
                def _():
                    dn_copy(i + dn_slots, slot).start()
                return 0
            lax.fori_loop(0, dn_steps, oth_step, 0)

            def fin(n, _):
                part_copy(1, n).wait()
                write(tp, h_ref, 1, n)
                return 0
            lax.fori_loop(0, dn_steps, fin, 0)
        else:
            def hop(buf, k, src, dst, peer):
                return send(src_ref=src, dst_ref=buf.at[dst], send_sem=wsem.at[0, k], recv_sem=wsem.at[1, k], device_id=peer)

            q_y = hop(wqn, 0, wq_ref.at[layer + 1, :, pl.ds(pl.multiple_of(sp * hd, hd), hd)], 0, other)
            o_y = hop(won, 1, wo_ref.at[layer + 1, pl.ds(pl.multiple_of(sp * hd, hd), hd), :], 0, other)
            q_hops = [hop(wqn, 2, wqn.at[0], 2, far), hop(wqn, 3, wqn.at[0], 1, mate)]
            o_hops = [hop(won, 4, won.at[0], 2, far), hop(won, 5, won.at[0], 1, mate)]
            q_last = hop(wqn, 6, wqn.at[2], 3, mate)
            o_last = hop(won, 7, won.at[2], 3, mate)

            h_copy.wait()
            q_y.start()
            o_y.start()
            norm(hoth)
            gate_up(gu_steps, 2 * gu_steps, 1)
            q_y.wait()
            for c in q_hops:
                c.start()

            def both_step(n, _):
                slot = lax.rem(n, dn_slots)
                dn_copy(n, slot).wait()
                sent[0, n] = dot32(a[1], dnb[slot]).astype(BF16)
                sent[1, n] = dot32(a[0], dnb[slot]).astype(BF16)
                part_copy(0, n).start()

                @pl.when(n + dn_slots < dn_steps)
                def _():
                    dn_copy(n + dn_slots, slot).start()
                return 0
            cut = dn_steps - 3
            lax.fori_loop(0, cut, both_step, 0)
            o_y.wait()
            for c in o_hops:
                c.start()
            lax.fori_loop(cut, dn_steps, both_step, 0)
            for c in q_hops:
                c.wait()
            q_last.start()

            def fin(n, _):
                part_copy(0, n).wait()
                mix = (sent[1, n].astype(F32) + got[0, n].astype(F32)).astype(BF16)
                out_ref[:, cols_of(n)] = (h_ref[:, cols_of(n)].astype(F32) + mix.astype(F32)).astype(BF16)
                return 0
            lax.fori_loop(0, dn_steps, fin, 0)
            for c in o_hops:
                c.wait()
            o_last.start()
            q_last.wait()
            o_last.wait()

    vmem = pl.BlockSpec(memory_space=pltpu.VMEM)
    sides = 1 if last else 2
    if last:
        outs = [jax.ShapeDtypeStruct((4, rows // 2, width), BF16)]
        out_specs = [vmem]
    else:
        outs = [jax.ShapeDtypeStruct((rows, width), BF16), jax.ShapeDtypeStruct((4, width, hd), BF16), jax.ShapeDtypeStruct((4, hd, width), BF16)]
        out_specs = [vmem, ANY, ANY]
    nsem = 2 if last else 1
    scratch = [
        pltpu.VMEM((rows, width), BF16), pltpu.VMEM((rows, width), BF16), pltpu.VMEM((sides, rows, ff), BF16),
        pltpu.VMEM((gu_slots, 2, width, bn), BF16), pltpu.VMEM((dn_slots, ff, dn), BF16),
        pltpu.VMEM((2, dn_steps, rows, dn), BF16), pltpu.VMEM((nsem, dn_steps, rows, dn), BF16),
        pltpu.SemaphoreType.DMA((gu_slots, 2)), pltpu.SemaphoreType.DMA((dn_slots,)), pltpu.SemaphoreType.DMA((2,)),
        pltpu.SemaphoreType.DMA((nsem, dn_steps)), pltpu.SemaphoreType.DMA((nsem, dn_steps)),
    ] + ([] if last else [pltpu.SemaphoreType.DMA((2, 8))])
    return pl.pallas_call(
        body, out_shape=outs, in_specs=[vmem, vmem] + [ANY] * 5, out_specs=out_specs, scratch_shapes=scratch,
        compiler_params=pltpu.CompilerParams(vmem_limit_bytes=62 * MIB, collective_id=layer, has_side_effects=True), name=f"mlp{layer}",
        cost_estimate=cost(12 * rows * width * ff, 10 * width * ff),
    )(h1, gain, w_gate, w_up, w_down, w_query, w_out)


def after(value, *deps):
    return lax.optimization_barrier((value,) + deps)[0]


def solution(mesh):
    sp_size = mesh.shape["sp"]
    tp_size = mesh.shape["tp"]
    in_specs = (P("dp", "sp", None), P("dp", "sp"), P("dp"), P(), P(), P("tp", None), P(), P(None, None, "tp"), P(), P(), P(None, "tp", None), P(), P(None, None, "tp"), P(None, None, "tp"), P(None, "tp", None))
    out_specs = (P("dp", "sp", None), P("dp", "sp", None), P(None, None, "dp", "sp", None), P(None, None, "dp", "sp", None))
    swap = lambda v: lax.ppermute(v, "tp", [(i, tp_size - 1 - i) for i in range(tp_size)])
    hop = lambda v, bit: lax.ppermute(v, "sp", [(i, i ^ bit) for i in range(sp_size)])

    def device_fn(features, tokens, lengths, proj_w, proj_b, embed, ln_attn, w_query, w_key, w_value, w_out, ln_mlp, w_gate, w_up, w_down):
        num_req, img_loc, _ = features.shape
        txt_loc = tokens.shape[1]
        seq = img_loc + txt_loc
        width = proj_w.shape[1]
        hd = w_key.shape[2]
        rows_loc = embed.shape[0]
        sp = lax.axis_index("sp")
        tp = lax.axis_index("tp")
        half = num_req // tp_size
        mine = lambda v, axis=0: lax.dynamic_slice_in_dim(v, tp * half, half, axis)
        theirs = lambda v, axis=0: lax.dynamic_slice_in_dim(v, (tp_size - 1 - tp) * half, half, axis)

        def rows_of(ids):
            return jnp.take(embed, jnp.clip(ids - tp * rows_loc, 0, rows_loc - 1).reshape(-1), axis=0, mode="clip")

        def start_of(feats, ids, rows, got):
            owned = (ids >= tp * rows_loc) & (ids < (tp + 1) * rows_loc)
            img = (jnp.einsum("bpc,cd->bpd", feats, proj_w, preferred_element_type=F32) + proj_b.astype(F32)).astype(BF16)
            picked = jnp.where(owned.reshape(-1)[:, None], rows, got)
            txt = (picked.astype(F32) * math.sqrt(width)).astype(BF16).reshape(half, txt_loc, width)
            return jnp.concatenate([img, txt], axis=1)

        my_ids, their_ids = mine(tokens), theirs(tokens)
        my_rows = rows_of(my_ids)
        their_got = swap(my_rows)
        their_rows = rows_of(after(their_ids, my_rows))
        my_got = swap(their_rows)

        positions = jnp.concatenate([sp * img_loc + jnp.arange(img_loc), img_loc * sp_size + sp * txt_loc + jnp.arange(txt_loc)])
        inv_freq = ROPE_THETA ** (-jnp.arange(hd // 2, dtype=F32) * (2.0 / hd))
        angles = positions.astype(F32)[:, None] * inv_freq[None, :]
        cos, sin = jnp.cos(angles), jnp.sin(angles)
        slot = jnp.arange(seq)[None, :]
        owner = jnp.stack([sp ^ b for b in range(sp_size)])[:, None]
        text_index = (owner * txt_loc + slot - img_loc).reshape(1, -1)
        is_img = jnp.broadcast_to(slot < img_loc, (sp_size, seq)).reshape(1, -1)
        mask_of = lambda lens: (is_img | (text_index < lens[:, None])).astype(F32)[:, None, :]
        my_mask, their_mask = mask_of(mine(lengths)), mask_of(theirs(lengths))

        def gather(kv):
            far = hop(kv, 2)
            return [kv, hop(kv, 1), far, hop(far, 1)]

        their_h = start_of(theirs(features), their_ids, their_rows, their_got)
        their_x, their_kv = kv_proj(0, their_h, ln_attn, w_key, w_value, cos, sin, "t")
        their_kvs = gather(their_kv)
        their_q = q_proj(0, their_x, w_query, None, cos, sin, "t")
        their_o = attend(0, their_q, their_kvs, their_mask, "t")
        back = swap(out_proj(0, their_o, w_out, None, None, None, "t"))
        hidden = start_of(mine(features), my_ids, my_rows, my_got)
        x, kv = kv_proj(0, hidden, ln_attn, w_key, w_value, cos, sin, "m")
        q = q_proj(0, x, w_query, None, cos, sin, "m")
        o = attend(0, q, gather(kv), my_mask, "m")
        h1 = out_proj(0, o, w_out, None, hidden, back, "m")
        caches = [(kv, their_kv)]
        flat = lambda v: v.reshape(half * seq, width)
        hidden, wq_next, wo_next = mlp(0, False, flat(h1), ln_mlp, w_gate, w_up, w_down, w_query, w_out)

        x, kv = kv_proj(1, hidden.reshape(half, seq, width), ln_attn, w_key, w_value, cos, sin, "m")
        kvs = gather(kv)
        q = q_proj(1, x, w_query, wq_next, cos, sin, "m")
        caches.append((kv, swap(kv)))
        o = attend(1, q, kvs, my_mask, "m")
        h1 = out_proj(1, o, w_out, wo_next, hidden.reshape(half, seq, width), None, "m")
        final, = mlp(1, True, flat(h1), ln_mlp, w_gate, w_up, w_down, w_query, w_out)

        def merge(a, b, axis):
            return jnp.where(tp == 0, jnp.concatenate([a, b], axis), jnp.concatenate([b, a], axis))

        cache = jnp.stack([merge(a, b, 1) for a, b in caches])
        return final[:, :img_loc], final[:, img_loc:], cache[:, :, :, :img_loc], cache[:, :, :, img_loc:]

    return jax.shard_map(device_fn, mesh=mesh, in_specs=in_specs, out_specs=out_specs, check_vma=False)
```

```python
import functools
import math
import jax
import jax.numpy as jnp
from jax import lax
from jax.experimental import pallas as pl
from jax.experimental.pallas import tpu as pltpu
from jax.sharding import PartitionSpec as P

NORM_EPS = 1e-6
ROPE_THETA = 10000.0
NUM_LAYERS = 2
F32 = jnp.float32
BF16 = jnp.bfloat16
MIB = 1024 * 1024
ANY = pl.BlockSpec(memory_space=pl.ANY)


def dot32(a, b):
    return jnp.dot(a, b, preferred_element_type=F32)


def rotate(vec, cos, sin):
    half = vec.shape[-1] // 2
    lo, hi = vec[:, :half], vec[:, half:]
    return jnp.concatenate([lo * cos - hi * sin, hi * cos + lo * sin], axis=-1)


def cost(flops, nbytes):
    return pl.CostEstimate(flops=int(flops), bytes_accessed=int(nbytes), transcendentals=0)


def normed(hid, gain):
    hid = hid.astype(F32)
    ms = jnp.mean(hid * hid, axis=-1, keepdims=True)
    return (hid * lax.rsqrt(ms + NORM_EPS) * (1.0 + gain.astype(F32))).astype(BF16)


def attention(layer, h, gain, w_key, w_value, w_query, w_out, pieces, cos, sin, mask, residual, tag, cid):
    rows, width = h.shape
    reqs = mask.shape[0]
    seq = rows // reqs
    hd = w_key.shape[2]
    local = w_query.shape[2] // hd
    heads = local * (1 if pieces is None else 2)
    srcs = mask.shape[2] // seq
    share = pieces is not None
    expo = hd ** -0.5 * math.log2(math.e)
    bn = 256
    steps = width // bn
    norm_rows = 48

    def body(h_ref, g_ref, cos_ref, sin_ref, mask_ref, wk_ref, wv_ref, wq_ref, wo_ref, *refs):
        if pieces is not None:
            wqn_ref, won_ref = refs[:2]
        kv_ref, y_ref, wkv, wqb, wob, x, q, kvb, p, o, wsem, osem, ssem, rsem = refs[0 if pieces is None else 2:]
        sp = lax.axis_index("sp")
        mate = {"sp": sp + 1 - 2 * lax.rem(sp, 2)}
        far = {"sp": lax.rem(sp + 2, 4)}
        tp = lax.axis_index("tp")
        place = tp if share else 0
        peers = (mate, far) + (({"tp": 1 - tp},) if share else ())

        def w_copy(i):
            if i < 2:
                return pltpu.make_async_copy((wk_ref, wv_ref)[i].at[layer], wkv.at[i], wsem.at[i])
            n = i - 2
            src = wq_ref.at[layer, :, pl.ds(n * hd, hd)] if n < local else wqn_ref.at[n - local]
            return pltpu.make_async_copy(src, wqb.at[n], wsem.at[i])

        def o_copies(n):
            cols = pl.ds(pl.multiple_of(n * bn, bn), bn)
            out = [pltpu.make_async_copy(wo_ref.at[layer, :, cols], wob.at[n, pl.ds(0, local * hd), :], osem.at[n, 0])]
            if pieces is not None:
                for i in range(local):
                    out.append(pltpu.make_async_copy(won_ref.at[i, :, cols], wob.at[n, pl.ds((local + i) * hd, hd), :], osem.at[n, 1 + i]))
            return out

        for i in range(2 + heads):
            w_copy(i).start()
        barrier = pltpu.get_barrier_semaphore()
        for peer in peers:
            pl.semaphore_signal(barrier, inc=1, device_id=peer, device_id_type=pl.DeviceIdType.MESH)

        def hop(k, slot, src, peer):
            return pltpu.make_async_remote_copy(src_ref=kvb.at[src, k], dst_ref=kvb.at[slot, k], send_sem=ssem.at[slot - 1, k],
                                                recv_sem=rsem.at[slot - 1, k], device_id=peer, device_id_type=pl.DeviceIdType.MESH)

        to_mate = [hop(k, 1, 0, mate) for k in range(2)]
        to_far = [hop(k, 2, 0, far) for k in range(2)]
        onward = [hop(k, 3, 2, mate) for k in range(2)]
        across = [pltpu.make_async_remote_copy(src_ref=kvb.at[0, k], dst_ref=kv_ref.at[k, tp], send_sem=ssem.at[3, k],
                                               recv_sem=rsem.at[3, k], device_id=peers[-1], device_id_type=pl.DeviceIdType.MESH)
                  for k in range(2 if share else 0)]

        def norm(i, _):
            r = pl.ds(pl.multiple_of(i * norm_rows, norm_rows), norm_rows)
            x[r, :] = normed(h_ref[r, :], g_ref[layer:layer + 1, :])
            return 0
        lax.fori_loop(0, rows // norm_rows, norm, 0)

        def turned(vec):
            return jnp.concatenate([rotate(vec[r * seq:(r + 1) * seq], cos_ref[...], sin_ref[...]) for r in range(reqs)], axis=0).astype(BF16)

        w_copy(0).wait()
        key = turned(dot32(x[...], wkv[0]))
        kvb[0, 0] = key
        kv_ref[0, place] = key
        w_copy(1).wait()
        val = dot32(x[...], wkv[1]).astype(BF16)
        kvb[0, 1] = val
        kv_ref[1, place] = val
        pl.semaphore_wait(barrier, len(peers))
        to_far[0].start()
        to_mate[0].start()

        def query(n, _):
            for i in range(heads):
                @pl.when(n == i)
                def _(i=i):
                    w_copy(2 + i).wait()
            q[n] = turned(dot32(x[...], wqb[n]))
            return 0

        lax.fori_loop(0, 1, query, 0)
        to_far[1].start()
        to_mate[1].start()
        for c in across:
            c.start()
        for n in range(steps):
            for c in o_copies(n):
                c.start()
        lax.fori_loop(1, heads, query, 0)
        to_far[0].wait_recv()
        onward[0].start()
        to_mate[0].wait_recv()
        onward[0].wait_recv()

        def probs(r):
            valid = mask_ref[r] > 0
            where = slice(r * seq, (r + 1) * seq)

            def step(n, _):
                k = jnp.concatenate([kvb[i, 0, where, :] for i in range(srcs)], axis=0)
                s = lax.dot_general(q[n, where, :], k, (((1,), (1,)), ((), ())), preferred_element_type=F32)
                s = jnp.where(valid, s, -1e30)
                top = jnp.max(s, axis=-1, keepdims=True)
                e = jnp.exp2((s - top) * expo)
                p[r, n] = (e * (1.0 / jnp.sum(e, axis=-1, keepdims=True))).astype(BF16)
                return 0
            lax.fori_loop(0, heads, step, 0)

        probs(0)
        to_far[1].wait_recv()
        onward[1].start()
        for r in range(1, reqs):
            probs(r)
        to_mate[1].wait_recv()
        onward[1].wait_recv()
        for r in range(reqs):
            where = slice(r * seq, (r + 1) * seq)
            v = jnp.concatenate([kvb[i, 1, where, :] for i in range(srcs)], axis=0)
            for n in range(0, heads, 2):
                got = dot32(p[r, n:n + 2].reshape(2 * seq, srcs * seq), v).astype(BF16)
                o[where, n * hd:(n + 1) * hd] = got[:seq]
                o[where, (n + 1) * hd:(n + 2) * hd] = got[seq:]

        def out_step(n, _):
            for c in o_copies(n):
                c.wait()
            cols = pl.ds(pl.multiple_of(n * bn, bn), bn)
            acc = dot32(o[...], wob[n]).astype(BF16)
            if residual:
                acc = (h_ref[:, cols].astype(F32) + acc.astype(F32)).astype(BF16)
            y_ref[:, cols] = acc
            return 0
        lax.fori_loop(0, steps, out_step, 0)
        for c in to_mate + to_far + onward:
            c.wait_send()
        for c in across:
            c.wait()

    vmem = pl.BlockSpec(memory_space=pltpu.VMEM)
    extra = [] if pieces is None else list(pieces)
    return pl.pallas_call(
        body, out_shape=[jax.ShapeDtypeStruct((2, 2 if share else 1, rows, hd), BF16), jax.ShapeDtypeStruct((rows, width), BF16)],
        in_specs=[vmem] * 5 + [ANY] * (4 + len(extra)), out_specs=[vmem, vmem],
        scratch_shapes=[
            pltpu.VMEM((2, width, hd), BF16), pltpu.VMEM((heads, width, hd), BF16), pltpu.VMEM((steps, heads * hd, bn), BF16),
            pltpu.VMEM((rows, width), BF16), pltpu.VMEM((heads, rows, hd), BF16), pltpu.VMEM((srcs, 2, rows, hd), BF16),
            pltpu.VMEM((reqs, heads, seq, srcs * seq), BF16), pltpu.VMEM((rows, heads * hd), BF16),
            pltpu.SemaphoreType.DMA((2 + heads,)), pltpu.SemaphoreType.DMA((steps, 5)),
            pltpu.SemaphoreType.DMA((4, 2)), pltpu.SemaphoreType.DMA((4, 2)),
        ],
        compiler_params=pltpu.CompilerParams(vmem_limit_bytes=58 * MIB, collective_id=cid, has_side_effects=True), name=f"attention{layer}{tag}",
        cost_estimate=cost(4 * rows * width * hd * (1 + heads) + 4 * rows * heads * hd * srcs * seq, 4 * heads * hd * width),
    )(h, gain, cos, sin, mask, w_key, w_value, w_query, w_out, *extra)


def mlp(layer, h1, gain, w_gate, w_up, w_down, w_query, w_out, splits=None):
    last = splits is not None
    rows, width = h1.shape
    ff = w_gate.shape[2]
    bn = 1024
    sub = 256
    gu_steps = ff // bn
    dn = 256
    dn_steps = width // dn
    gu_slots, dn_slots = 2, 3
    norm_rows = 48
    hd = 256

    def body(h_ref, g_ref, wg_ref, wu_ref, wd_ref, wq_ref, wo_ref, *refs):
        if last:
            img_ref, txt_ref, hoth, x, a, gub, dnb, sent, got, gsem, dsem, hsem, ssem, rsem = refs
        else:
            out_ref, wqn, won, hoth, x, a, gub, dnb, sent, got, gsem, dsem, hsem, ssem, rsem, wsem = refs
        tp = lax.axis_index("tp")
        sp = lax.axis_index("sp")
        other = {"tp": 1 - tp}
        mate = {"sp": sp + 1 - 2 * lax.rem(sp, 2)}
        far = {"sp": lax.rem(sp + 2, 4)}
        peers = [other] if last else [other, mate, far]
        send = functools.partial(pltpu.make_async_remote_copy, device_id_type=pl.DeviceIdType.MESH)

        def gu_copies(i, slot):
            cols = pl.ds(pl.multiple_of(lax.rem(i, gu_steps) * bn, bn), bn)
            return [pltpu.make_async_copy(w.at[layer, :, cols], gub.at[slot, k], gsem.at[slot, k]) for k, w in enumerate((wg_ref, wu_ref))]

        def dn_copy(i, slot):
            cols = pl.ds(pl.multiple_of(lax.rem(i, dn_steps) * dn, dn), dn)
            return pltpu.make_async_copy(wd_ref.at[layer, :, cols], dnb.at[slot], dsem.at[slot])

        for i in range(gu_slots):
            for c in gu_copies(i, i):
                c.start()
        for i in range(dn_slots):
            dn_copy(i, i).start()
        barrier = pltpu.get_barrier_semaphore()
        for peer in peers:
            pl.semaphore_signal(barrier, inc=1, device_id=peer, device_id_type=pl.DeviceIdType.MESH)
        pl.semaphore_wait(barrier, len(peers))
        h_copy = send(src_ref=h_ref, dst_ref=hoth, send_sem=hsem.at[0], recv_sem=hsem.at[1], device_id=other)
        h_copy.start()

        def norm(src):
            def step(i, _):
                r = pl.ds(pl.multiple_of(i * norm_rows, norm_rows), norm_rows)
                x[r, :] = normed(src[r, :], g_ref[layer:layer + 1, :])
                return 0
            lax.fori_loop(0, rows // norm_rows, step, 0)

        def gate_up(i, side):
            slot = lax.rem(i, gu_slots)
            for cp in gu_copies(i, slot):
                cp.wait()
            for j in range(bn // sub):
                cols = slice(j * sub, (j + 1) * sub)
                gate = dot32(x[...], gub[slot, 0, :, cols])
                up = dot32(x[...], gub[slot, 1, :, cols])
                mix = (jax.nn.gelu(gate, approximate=True) * up).astype(BF16)
                a[side, :, pl.ds(pl.multiple_of(lax.rem(i, gu_steps) * bn + j * sub, sub), sub)] = mix

            @pl.when(i + gu_slots < 2 * gu_steps)
            def _():
                for cp in gu_copies(i + gu_slots, slot):
                    cp.start()

        def part_copy(k, n):
            return send(src_ref=sent.at[k, n], dst_ref=got.at[k, n], send_sem=ssem.at[k, n], recv_sem=rsem.at[k, n], device_id=other)

        def cols_of(n):
            return pl.ds(pl.multiple_of(n * dn, dn), dn)

        norm(h_ref)
        if last:
            reqs = img_ref.shape[0] // 2
            img = img_ref.shape[1]
            seq = img + txt_ref.shape[1]

            def write(first, src, k, n):
                mix = (sent[1 - k, n].astype(F32) + got[k, n].astype(F32)).astype(BF16)
                y = (src[:, cols_of(n)].astype(F32) + mix.astype(F32)).astype(BF16).reshape(reqs, seq, dn)
                img_ref[pl.ds(first * reqs, reqs), :, cols_of(n)] = y[:, :img]
                txt_ref[pl.ds(first * reqs, reqs), :, cols_of(n)] = y[:, img:]

            def side_step(side, _):
                @pl.when(side == 1)
                def _():
                    h_copy.wait()
                    part_copy(0, dn_steps - 1).start()
                    norm(hoth)

                def gu_step(c, _):
                    gate_up(side * gu_steps + c, 0)
                    return 0
                lax.fori_loop(0, gu_steps, gu_step, 0)

                def dn_step(n, _):
                    i = side * dn_steps + n
                    slot = lax.rem(i, dn_slots)
                    dn_copy(i, slot).wait()
                    sent[side, n] = dot32(a[0], dnb[slot]).astype(BF16)

                    @pl.when(i + dn_slots < 2 * dn_steps)
                    def _():
                        dn_copy(i + dn_slots, slot).start()

                    @pl.when((side == 0) & (n > 0))
                    def _():
                        part_copy(0, n - 1).start()

                    @pl.when(side == 1)
                    def _():
                        part_copy(0, n).wait()
                        write(1 - tp, hoth, 0, n)
                        part_copy(1, n).start()
                    return 0
                lax.fori_loop(0, dn_steps, dn_step, 0)
                return 0
            lax.fori_loop(0, 2, side_step, 0)

            def fin(n, _):
                part_copy(1, n).wait()
                write(tp, h_ref, 1, n)
                return 0
            lax.fori_loop(0, dn_steps, fin, 0)
        else:
            def hop(buf, k, src, dst, peer):
                return send(src_ref=src, dst_ref=buf.at[dst], send_sem=wsem.at[0, k], recv_sem=wsem.at[1, k], device_id=peer)

            q_y = hop(wqn, 0, wq_ref.at[layer + 1, :, pl.ds(pl.multiple_of(sp * hd, hd), hd)], 0, other)
            o_y = hop(won, 1, wo_ref.at[layer + 1, pl.ds(pl.multiple_of(sp * hd, hd), hd), :], 0, other)
            q_hops = [hop(wqn, 2, wqn.at[0], 2, far), hop(wqn, 3, wqn.at[0], 1, mate)]
            o_hops = [hop(won, 4, won.at[0], 2, far), hop(won, 5, won.at[0], 1, mate)]
            q_last = hop(wqn, 6, wqn.at[2], 3, mate)
            o_last = hop(won, 7, won.at[2], 3, mate)

            def gu_step(i, _):
                @pl.when(i == gu_steps)
                def _():
                    h_copy.wait()
                    q_y.start()
                    o_y.start()
                    norm(hoth)
                gate_up(i, lax.div(i, gu_steps))
                return 0
            lax.fori_loop(0, 2 * gu_steps, gu_step, 0)
            q_y.wait()
            for c in q_hops:
                c.start()

            def both_step(n, _):
                @pl.when(n == dn_steps - 3)
                def _():
                    o_y.wait()
                    for c in o_hops:
                        c.start()
                slot = lax.rem(n, dn_slots)
                dn_copy(n, slot).wait()
                sent[0, n] = dot32(a[1], dnb[slot]).astype(BF16)
                sent[1, n] = dot32(a[0], dnb[slot]).astype(BF16)
                part_copy(0, n).start()

                @pl.when(n + dn_slots < dn_steps)
                def _():
                    dn_copy(n + dn_slots, slot).start()
                return 0
            lax.fori_loop(0, dn_steps, both_step, 0)
            for c in q_hops:
                c.wait()
            q_last.start()

            def fin(n, _):
                part_copy(0, n).wait()
                mix = (sent[1, n].astype(F32) + got[0, n].astype(F32)).astype(BF16)
                out_ref[:, cols_of(n)] = (h_ref[:, cols_of(n)].astype(F32) + mix.astype(F32)).astype(BF16)
                return 0
            lax.fori_loop(0, dn_steps, fin, 0)
            for c in o_hops:
                c.wait()
            o_last.start()
            q_last.wait()
            o_last.wait()

    vmem = pl.BlockSpec(memory_space=pltpu.VMEM)
    sides = 1 if last else 2
    if last:
        outs = [jax.ShapeDtypeStruct((4, n, width), BF16) for n in splits]
        out_specs = [vmem, vmem]
    else:
        outs = [jax.ShapeDtypeStruct((rows, width), BF16), jax.ShapeDtypeStruct((4, width, hd), BF16), jax.ShapeDtypeStruct((4, hd, width), BF16)]
        out_specs = [vmem, ANY, ANY]
    nsem = 2 if last else 1
    scratch = [
        pltpu.VMEM((rows, width), BF16), pltpu.VMEM((rows, width), BF16), pltpu.VMEM((sides, rows, ff), BF16),
        pltpu.VMEM((gu_slots, 2, width, bn), BF16), pltpu.VMEM((dn_slots, ff, dn), BF16),
        pltpu.VMEM((2, dn_steps, rows, dn), BF16), pltpu.VMEM((nsem, dn_steps, rows, dn), BF16),
        pltpu.SemaphoreType.DMA((gu_slots, 2)), pltpu.SemaphoreType.DMA((dn_slots,)), pltpu.SemaphoreType.DMA((2,)),
        pltpu.SemaphoreType.DMA((nsem, dn_steps)), pltpu.SemaphoreType.DMA((nsem, dn_steps)),
    ] + ([] if last else [pltpu.SemaphoreType.DMA((2, 8))])
    return pl.pallas_call(
        body, out_shape=outs, in_specs=[vmem, vmem] + [ANY] * 5, out_specs=out_specs, scratch_shapes=scratch,
        compiler_params=pltpu.CompilerParams(vmem_limit_bytes=62 * MIB, collective_id=layer, has_side_effects=True), name=f"mlp{layer}",
        cost_estimate=cost(12 * rows * width * ff, 10 * width * ff),
    )(h1, gain, w_gate, w_up, w_down, w_query, w_out)


def after(value, *deps):
    return lax.optimization_barrier((value,) + deps)[0]


def solution(mesh):
    sp_size = mesh.shape["sp"]
    tp_size = mesh.shape["tp"]
    in_specs = (P("dp", "sp", None), P("dp", "sp"), P("dp"), P(), P(), P("tp", None), P(), P(None, None, "tp"), P(), P(), P(None, "tp", None), P(), P(None, None, "tp"), P(None, None, "tp"), P(None, "tp", None))
    out_specs = (P("dp", "sp", None), P("dp", "sp", None), P(None, None, "dp", "sp", None), P(None, None, "dp", "sp", None))
    swap = lambda v: lax.ppermute(v, "tp", [(i, tp_size - 1 - i) for i in range(tp_size)])

    def device_fn(features, tokens, lengths, proj_w, proj_b, embed, ln_attn, w_query, w_key, w_value, w_out, ln_mlp, w_gate, w_up, w_down):
        num_req, img_loc, _ = features.shape
        txt_loc = tokens.shape[1]
        seq = img_loc + txt_loc
        width = proj_w.shape[1]
        hd = w_key.shape[2]
        rows_loc = embed.shape[0]
        sp = lax.axis_index("sp")
        tp = lax.axis_index("tp")
        half = num_req // tp_size
        mine = lambda v, axis=0: lax.dynamic_slice_in_dim(v, tp * half, half, axis)
        theirs = lambda v, axis=0: lax.dynamic_slice_in_dim(v, (tp_size - 1 - tp) * half, half, axis)

        def rows_of(ids):
            return jnp.take(embed, jnp.clip(ids - tp * rows_loc, 0, rows_loc - 1), axis=0, mode="clip")

        def start_of(feats, ids, rows, got):
            owned = (ids >= tp * rows_loc) & (ids < (tp + 1) * rows_loc)
            img = (jnp.einsum("bpc,cd->bpd", feats, proj_w, preferred_element_type=F32) + proj_b.astype(F32)).astype(BF16)
            parts = []
            for r in range(half):
                picked = jnp.where(owned[r][:, None], rows[r], got[r])
                parts += [img[r], (picked.astype(F32) * math.sqrt(width)).astype(BF16)]
            return jnp.concatenate(parts, axis=0)

        my_ids, their_ids = mine(tokens), theirs(tokens)
        picks, sent = [], []
        for ids in (my_ids[0], my_ids[1], their_ids[0], their_ids[1]):
            picks.append(rows_of(after(ids, *picks[-1:])))
            sent.append(swap(picks[-1]))

        positions = jnp.concatenate([sp * img_loc + jnp.arange(img_loc), img_loc * sp_size + sp * txt_loc + jnp.arange(txt_loc)])
        inv_freq = ROPE_THETA ** (-jnp.arange(hd // 2, dtype=F32) * (2.0 / hd))
        angles = positions.astype(F32)[:, None] * inv_freq[None, :]
        cos, sin = jnp.cos(angles), jnp.sin(angles)
        slot = jnp.arange(seq)[None, :]
        owner = jnp.stack([sp ^ b for b in range(sp_size)])[:, None]
        text_index = (owner * txt_loc + slot - img_loc).reshape(1, -1)
        is_img = jnp.broadcast_to(slot < img_loc, (sp_size, seq)).reshape(1, -1)
        mask_of = lambda lens: (is_img | (text_index < lens[:, None])).astype(F32)[:, None, :]
        my_mask, their_mask = mask_of(mine(lengths)), mask_of(theirs(lengths))

        weights = (w_key, w_value, w_query, w_out)
        their_h = start_of(theirs(features), their_ids, picks[2:], sent[:2])
        their_kv, their_part = attention(0, their_h, ln_attn, *weights, None, cos, sin, their_mask, False, "t", 2)
        back = swap(their_part)
        hidden = start_of(mine(features), my_ids, picks[:2], sent[2:])
        kv, part = attention(0, hidden, ln_attn, *weights, None, cos, sin, my_mask, False, "m", 3)
        part = (part.astype(F32) + back.astype(F32)).astype(BF16)
        h1 = (hidden.astype(F32) + part.astype(F32)).astype(BF16)
        pair = [v.reshape(2, half, seq, hd) for v in (kv, their_kv)]
        caches = [jnp.where(tp == 0, jnp.concatenate(pair, axis=1), jnp.concatenate(pair[::-1], axis=1))]
        hidden, wq_next, wo_next = mlp(0, h1, ln_mlp, w_gate, w_up, w_down, w_query, w_out)

        kv, h1 = attention(1, hidden, ln_attn, *weights, (wq_next, wo_next), cos, sin, my_mask, True, "m", 4)
        caches.append(kv.reshape(2, num_req, seq, hd))
        final = mlp(1, h1, ln_mlp, w_gate, w_up, w_down, w_query, w_out, splits=(img_loc, txt_loc))

        cache = jnp.stack(caches)
        return final[0], final[1], cache[:, :, :, :img_loc], cache[:, :, :, img_loc:]

    return jax.shard_map(device_fn, mesh=mesh, in_specs=in_specs, out_specs=out_specs, check_vma=False)
```

```python
import functools
import math
import jax
import jax.numpy as jnp
from jax import lax
from jax.experimental import pallas as pl
from jax.experimental.pallas import tpu as pltpu
from jax.sharding import PartitionSpec as P

NORM_EPS = 1e-6
ROPE_THETA = 10000.0
NUM_LAYERS = 2
F32 = jnp.float32
BF16 = jnp.bfloat16
MIB = 1024 * 1024
ANY = pl.BlockSpec(memory_space=pl.ANY)


def dot32(a, b):
    return jnp.dot(a, b, preferred_element_type=F32)


def rotate(vec, cos, sin):
    half = vec.shape[-1] // 2
    lo, hi = vec[:, :half], vec[:, half:]
    return jnp.concatenate([lo * cos - hi * sin, hi * cos + lo * sin], axis=-1)


def cost(flops, nbytes):
    return pl.CostEstimate(flops=int(flops), bytes_accessed=int(nbytes), transcendentals=0)


def normed(hid, gain):
    hid = hid.astype(F32)
    ms = jnp.mean(hid * hid, axis=-1, keepdims=True)
    return (hid * lax.rsqrt(ms + NORM_EPS) * (1.0 + gain.astype(F32))).astype(BF16)


def attention(layer, h, gain, w_key, w_value, w_query, w_out, pieces, cos, sin, mask, tag, cid, keep=False, ahead=False):
    first = isinstance(h, tuple)
    residual = not first
    width = w_query.shape[1]
    reqs = mask.shape[0]
    if first:
        img_loc, txt_loc = h[0].shape[1], h[1].shape[0]
        rows = reqs * (img_loc + txt_loc)
    else:
        rows = h.shape[0]
    seq = rows // reqs
    hd = w_key.shape[2]
    local = w_query.shape[2] // hd
    heads = local * (1 if pieces is None else 2)
    srcs = mask.shape[2] // seq
    share = pieces is not None
    expo = hd ** -0.5 * math.log2(math.e)
    bn = 256
    steps = width // bn
    norm_rows = 48

    ins = list(h) if first else [h]

    def body(*refs):
        h_refs, refs = refs[:len(ins)], refs[len(ins):]
        g_ref, cos_ref, sin_ref, mask_ref, wk_ref, wv_ref, wq_ref, wo_ref = refs[:8]
        refs = refs[8:]
        if pieces is not None:
            wqn_ref, won_ref, wqh_ref = refs[:3]
            refs = refs[3:]
        kv_ref, y_ref = refs[:2]
        refs = refs[2:]
        if ahead:
            half_ref, refs = refs[0], refs[1:]
        if first:
            h_ref, refs = refs[0], refs[1:]
        else:
            h_ref = h_refs[0]
        wkv, wqb, wob, x, q, kvb, p, o, wsem, osem, ssem, rsem = refs
        sp = lax.axis_index("sp")
        mate = {"sp": sp + 1 - 2 * lax.rem(sp, 2)}
        far = {"sp": lax.rem(sp + 2, 4)}
        tp = lax.axis_index("tp")
        place = tp if share else 0
        peers = (mate, far) + (({"tp": 1 - tp},) if share or ahead else ())

        def w_copy(i):
            if i < 2:
                return pltpu.make_async_copy((wk_ref, wv_ref)[i].at[layer], wkv.at[i], wsem.at[i])
            n = i - 2
            if n < local:
                return pltpu.make_async_copy(wq_ref.at[layer, :, pl.ds(n * hd, hd)], wqb.at[n], wsem.at[i])
            if n == local:
                low = pl.ds(width // 2, width // 2)
                return pltpu.make_async_copy(wqn_ref.at[0, low, :], wqb.at[n, low, :], wsem.at[i])
            return pltpu.make_async_copy(wqn_ref.at[n - local], wqb.at[n], wsem.at[i])

        def top_copy():
            return pltpu.make_async_copy(wqh_ref, wqb.at[local, pl.ds(0, width // 2), :], wsem.at[2 + heads])

        def o_copies(n):
            cols = pl.ds(pl.multiple_of(n * bn, bn), bn)
            out = [pltpu.make_async_copy(wo_ref.at[layer, :, cols], wob.at[n, pl.ds(0, local * hd), :], osem.at[n, 0])]
            if pieces is not None:
                for i in range(local):
                    out.append(pltpu.make_async_copy(won_ref.at[i, :, cols], wob.at[n, pl.ds((local + i) * hd, hd), :], osem.at[n, 1 + i]))
            return out

        for i in range(2 + heads):
            w_copy(i).start()
        if pieces is not None:
            top_copy().start()
        barrier = pltpu.get_barrier_semaphore()
        for peer in peers:
            pl.semaphore_signal(barrier, inc=1, device_id=peer, device_id_type=pl.DeviceIdType.MESH)

        def hop(k, slot, src, peer):
            return pltpu.make_async_remote_copy(src_ref=kvb.at[src, k], dst_ref=kvb.at[slot, k], send_sem=ssem.at[slot - 1, k],
                                                recv_sem=rsem.at[slot - 1, k], device_id=peer, device_id_type=pl.DeviceIdType.MESH)

        to_mate = [hop(k, 1, 0, mate) for k in range(2)]
        to_far = [hop(k, 2, 0, far) for k in range(2)]
        onward = [hop(k, 3, 2, mate) for k in range(2)]
        across = [pltpu.make_async_remote_copy(src_ref=kvb.at[0, k], dst_ref=kv_ref.at[k, tp], send_sem=ssem.at[3, k],
                                               recv_sem=rsem.at[3, k], device_id=peers[-1], device_id_type=pl.DeviceIdType.MESH)
                  for k in range(2 if share else 0)]
        if ahead:
            src = wq_ref.at[layer + 1, pl.ds(0, width // 2), pl.ds(pl.multiple_of(sp * hd, hd), hd)]
            across = [pltpu.make_async_remote_copy(src_ref=src, dst_ref=half_ref, send_sem=ssem.at[3, 0], recv_sem=rsem.at[3, 0],
                                                   device_id=peers[-1], device_id_type=pl.DeviceIdType.MESH)]
        if first:
            img_ref, own_refs, got_refs, owned_ref = h_refs[0], h_refs[1:1 + reqs], h_refs[1 + reqs:1 + 2 * reqs], h_refs[-1]
            for r in range(reqs):
                h_ref[r * seq:r * seq + img_loc, :] = img_ref[r]
                for j in range(0, txt_loc, 64):
                    at = slice(j, j + 64)
                    picked = jnp.where(owned_ref[r, at, :] > 0, own_refs[r][at, :].astype(F32), got_refs[r][at, :].astype(F32))
                    h_ref[r * seq + img_loc + j:r * seq + img_loc + j + 64, :] = (picked * math.sqrt(width)).astype(BF16)

        def norm(i, _):
            r = pl.ds(pl.multiple_of(i * norm_rows, norm_rows), norm_rows)
            x[r, :] = normed(h_ref[r, :], g_ref[layer:layer + 1, :])
            return 0
        lax.fori_loop(0, rows // norm_rows, norm, 0)

        def turned(vec):
            return jnp.concatenate([rotate(vec[r * seq:(r + 1) * seq], cos_ref[...], sin_ref[...]) for r in range(reqs)], axis=0).astype(BF16)

        w_copy(0).wait()
        key = turned(dot32(x[...], wkv[0]))
        kvb[0, 0] = key
        kv_ref[0, place] = key
        w_copy(1).wait()
        val = dot32(x[...], wkv[1]).astype(BF16)
        kvb[0, 1] = val
        kv_ref[1, place] = val
        pl.semaphore_wait(barrier, len(peers))
        to_far[0].start()
        to_mate[0].start()

        def query(n, _):
            for i in range(heads):
                @pl.when(n == i)
                def _(i=i):
                    w_copy(2 + i).wait()
                    if pieces is not None and i == local:
                        top_copy().wait()
            q[n] = turned(dot32(x[...], wqb[n]))
            return 0

        lax.fori_loop(0, 1, query, 0)
        to_far[1].start()
        to_mate[1].start()
        for c in across:
            c.start()
        for n in range(steps):
            for c in o_copies(n):
                c.start()
        lax.fori_loop(1, heads, query, 0)
        to_far[0].wait_recv()
        onward[0].start()
        to_mate[0].wait_recv()
        onward[0].wait_recv()

        def probs(r):
            valid = mask_ref[r] > 0
            where = slice(r * seq, (r + 1) * seq)

            def step(n, _):
                k = jnp.concatenate([kvb[i, 0, where, :] for i in range(srcs)], axis=0)
                s = lax.dot_general(q[n, where, :], k, (((1,), (1,)), ((), ())), preferred_element_type=F32)
                s = jnp.where(valid, s, -1e30)
                top = jnp.max(s, axis=-1, keepdims=True)
                e = jnp.exp2((s - top) * expo)
                p[r, n] = (e * (1.0 / jnp.sum(e, axis=-1, keepdims=True))).astype(BF16)
                return 0
            lax.fori_loop(0, heads, step, 0)

        probs(0)
        to_far[1].wait_recv()
        onward[1].start()
        for r in range(1, reqs):
            probs(r)
        to_mate[1].wait_recv()
        onward[1].wait_recv()
        for r in range(reqs):
            where = slice(r * seq, (r + 1) * seq)
            v = jnp.concatenate([kvb[i, 1, where, :] for i in range(srcs)], axis=0)
            for n in range(0, heads, 2):
                got = dot32(p[r, n:n + 2].reshape(2 * seq, srcs * seq), v).astype(BF16)
                o[where, n * hd:(n + 1) * hd] = got[:seq]
                o[where, (n + 1) * hd:(n + 2) * hd] = got[seq:]

        def out_step(n, _):
            for c in o_copies(n):
                c.wait()
            cols = pl.ds(pl.multiple_of(n * bn, bn), bn)
            acc = dot32(o[...], wob[n]).astype(BF16)
            if residual:
                acc = (h_ref[:, cols].astype(F32) + acc.astype(F32)).astype(BF16)
            y_ref[:, cols] = acc
            return 0
        lax.fori_loop(0, steps, out_step, 0)
        for c in to_mate + to_far + onward:
            c.wait_send()
        for c in across:
            c.wait()

    vmem = pl.BlockSpec(memory_space=pltpu.VMEM)
    extra = [] if pieces is None else list(pieces)
    outs = [jax.ShapeDtypeStruct((2, 2 if share else 1, rows, hd), BF16), jax.ShapeDtypeStruct((rows, width), BF16)]
    out_specs = [vmem, vmem]
    if ahead:
        outs.append(jax.ShapeDtypeStruct((width // 2, hd), BF16))
        out_specs.append(ANY)
    if keep:
        outs.append(jax.ShapeDtypeStruct((rows, width), BF16))
        out_specs.append(vmem)
    return pl.pallas_call(
        body, out_shape=outs, in_specs=[vmem] * (len(ins) + 4) + [ANY] * (4 + len(extra)), out_specs=out_specs,
        scratch_shapes=([pltpu.VMEM((rows, width), BF16)] if first and not keep else []) + [
            pltpu.VMEM((2, width, hd), BF16), pltpu.VMEM((heads, width, hd), BF16), pltpu.VMEM((steps, heads * hd, bn), BF16),
            pltpu.VMEM((rows, width), BF16), pltpu.VMEM((heads, rows, hd), BF16), pltpu.VMEM((srcs, 2, rows, hd), BF16),
            pltpu.VMEM((reqs, heads, seq, srcs * seq), BF16), pltpu.VMEM((rows, heads * hd), BF16),
            pltpu.SemaphoreType.DMA((3 + heads,)), pltpu.SemaphoreType.DMA((steps, 5)),
            pltpu.SemaphoreType.DMA((4, 2)), pltpu.SemaphoreType.DMA((4, 2)),
        ],
        compiler_params=pltpu.CompilerParams(vmem_limit_bytes=58 * MIB, collective_id=cid, has_side_effects=True), name=f"attention{layer}{tag}",
        cost_estimate=cost(4 * rows * width * hd * (1 + heads) + 4 * rows * heads * hd * srcs * seq, 4 * heads * hd * width),
    )(*ins, gain, cos, sin, mask, w_key, w_value, w_query, w_out, *extra)


def mlp(layer, h1, gain, w_gate, w_up, w_down, w_query, w_out, wq_half=None, splits=None):
    last = splits is not None
    rows, width = h1.shape if last else h1[0].shape
    ff = w_gate.shape[2]
    bn = 1024
    sub = 256
    gu_steps = ff // bn
    dn = 256
    dn_steps = width // dn
    gu_slots, dn_slots = 2, 3
    norm_rows = 48
    hd = 256

    ins = [h1] if last else list(h1)

    def body(*refs):
        h_refs, refs = refs[:len(ins)], refs[len(ins):]
        g_ref, wg_ref, wu_ref, wd_ref, wq_ref, wo_ref = refs[:6]
        refs = refs[6:]
        if last:
            h_ref = h_refs[0]
            img_ref, txt_ref, hoth, x, a, gub, dnb, sent, got, gsem, dsem, hsem, ssem, rsem = refs
        else:
            wqh_ref, out_ref, wqn, won, h_ref, hoth, x, a, gub, dnb, sent, got, gsem, dsem, hsem, ssem, rsem, wsem = refs
        tp = lax.axis_index("tp")
        sp = lax.axis_index("sp")
        other = {"tp": 1 - tp}
        mate = {"sp": sp + 1 - 2 * lax.rem(sp, 2)}
        far = {"sp": lax.rem(sp + 2, 4)}
        peers = [other] if last else [other, mate, far]
        send = functools.partial(pltpu.make_async_remote_copy, device_id_type=pl.DeviceIdType.MESH)

        def gu_copies(i, slot):
            cols = pl.ds(pl.multiple_of(lax.rem(i, gu_steps) * bn, bn), bn)
            return [pltpu.make_async_copy(w.at[layer, :, cols], gub.at[slot, k], gsem.at[slot, k]) for k, w in enumerate((wg_ref, wu_ref))]

        def dn_copy(i, slot):
            cols = pl.ds(pl.multiple_of(lax.rem(i, dn_steps) * dn, dn), dn)
            return pltpu.make_async_copy(wd_ref.at[layer, :, cols], dnb.at[slot], dsem.at[slot])

        for i in range(gu_slots):
            for c in gu_copies(i, i):
                c.start()
        for i in range(dn_slots):
            dn_copy(i, i).start()
        barrier = pltpu.get_barrier_semaphore()
        for peer in peers:
            pl.semaphore_signal(barrier, inc=1, device_id=peer, device_id_type=pl.DeviceIdType.MESH)
        if not last:
            def total(i, _):
                r = pl.ds(pl.multiple_of(i * norm_rows, norm_rows), norm_rows)
                part = (h_refs[1][r, :].astype(F32) + h_refs[2][r, :].astype(F32)).astype(BF16)
                h_ref[r, :] = (h_refs[0][r, :].astype(F32) + part.astype(F32)).astype(BF16)
                return 0
            lax.fori_loop(0, rows // norm_rows, total, 0)
        pl.semaphore_wait(barrier, len(peers))
        h_copy = send(src_ref=h_ref, dst_ref=hoth, send_sem=hsem.at[0], recv_sem=hsem.at[1], device_id=other)
        if last:
            h_copy.start()

        def norm(src):
            def step(i, _):
                r = pl.ds(pl.multiple_of(i * norm_rows, norm_rows), norm_rows)
                x[r, :] = normed(src[r, :], g_ref[layer:layer + 1, :])
                return 0
            lax.fori_loop(0, rows // norm_rows, step, 0)

        def gate_up(i, side):
            slot = lax.rem(i, gu_slots)
            for cp in gu_copies(i, slot):
                cp.wait()
            for j in range(bn // sub):
                cols = slice(j * sub, (j + 1) * sub)
                gate = dot32(x[...], gub[slot, 0, :, cols])
                up = dot32(x[...], gub[slot, 1, :, cols])
                mix = (jax.nn.gelu(gate, approximate=True) * up).astype(BF16)
                a[side, :, pl.ds(pl.multiple_of(lax.rem(i, gu_steps) * bn + j * sub, sub), sub)] = mix

            @pl.when(i + gu_slots < 2 * gu_steps)
            def _():
                for cp in gu_copies(i + gu_slots, slot):
                    cp.start()

        def part_copy(k, n):
            return send(src_ref=sent.at[k, n], dst_ref=got.at[k, n], send_sem=ssem.at[k, n], recv_sem=rsem.at[k, n], device_id=other)

        def cols_of(n):
            return pl.ds(pl.multiple_of(n * dn, dn), dn)

        norm(h_ref)
        if not last:
            h_copy.start()
        if last:
            reqs = img_ref.shape[0] // 2
            img = img_ref.shape[1]
            seq = img + txt_ref.shape[1]

            def write(first, src, k, n):
                mix = (sent[1 - k, n].astype(F32) + got[k, n].astype(F32)).astype(BF16)
                y = (src[:, cols_of(n)].astype(F32) + mix.astype(F32)).astype(BF16).reshape(reqs, seq, dn)
                img_ref[pl.ds(first * reqs, reqs), :, cols_of(n)] = y[:, :img]
                txt_ref[pl.ds(first * reqs, reqs), :, cols_of(n)] = y[:, img:]

            def side_step(side, _):
                @pl.when(side == 1)
                def _():
                    h_copy.wait()
                    part_copy(0, dn_steps - 1).start()
                    norm(hoth)

                def gu_step(c, _):
                    gate_up(side * gu_steps + c, 0)
                    return 0
                lax.fori_loop(0, gu_steps, gu_step, 0)

                def dn_step(n, _):
                    i = side * dn_steps + n
                    slot = lax.rem(i, dn_slots)
                    dn_copy(i, slot).wait()
                    sent[side, n] = dot32(a[0], dnb[slot]).astype(BF16)

                    @pl.when(i + dn_slots < 2 * dn_steps)
                    def _():
                        dn_copy(i + dn_slots, slot).start()

                    @pl.when((side == 0) & (n > 0))
                    def _():
                        part_copy(0, n - 1).start()

                    @pl.when(side == 1)
                    def _():
                        part_copy(0, n).wait()
                        write(1 - tp, hoth, 0, n)
                        part_copy(1, n).start()
                    return 0
                lax.fori_loop(0, dn_steps, dn_step, 0)
                return 0
            lax.fori_loop(0, 2, side_step, 0)

            def fin(n, _):
                part_copy(1, n).wait()
                write(tp, h_ref, 1, n)
                return 0
            lax.fori_loop(0, dn_steps, fin, 0)
        else:
            def hop(k, src, dst, peer):
                return send(src_ref=src, dst_ref=dst, send_sem=wsem.at[0, k], recv_sem=wsem.at[1, k], device_id=peer)

            low, high = pl.ds(0, width // 2), pl.ds(width // 2, width // 2)
            q_y = hop(0, wq_ref.at[layer + 1, high, pl.ds(pl.multiple_of(sp * hd, hd), hd)], wqn.at[0, high, :], other)
            o_y = hop(1, wo_ref.at[layer + 1, pl.ds(pl.multiple_of(sp * hd, hd), hd), :], won.at[0], other)
            q_hops = [hop(2, wqn.at[0, high, :], wqn.at[2, high, :], far), hop(3, wqn.at[0, high, :], wqn.at[1, high, :], mate)]
            o_hops = [hop(4, won.at[0], won.at[2], far), hop(5, won.at[0], won.at[1], mate)]
            q_last = hop(6, wqn.at[2, high, :], wqn.at[3, high, :], mate)
            o_last = hop(7, won.at[2], won.at[3], mate)
            t_hops = [hop(8, wqh_ref, wqn.at[2, low, :], far), hop(9, wqh_ref, wqn.at[1, low, :], mate)]
            t_last = hop(10, wqn.at[2, low, :], wqn.at[3, low, :], mate)
            for c in t_hops:
                c.start()

            def gu_step(i, _):
                @pl.when(i == gu_steps)
                def _():
                    h_copy.wait()
                    q_y.start()
                    o_y.start()
                    for c in t_hops:
                        c.wait()
                    t_last.start()
                    norm(hoth)
                gate_up(i, lax.div(i, gu_steps))
                return 0
            lax.fori_loop(0, 2 * gu_steps, gu_step, 0)
            q_y.wait()
            for c in q_hops:
                c.start()

            def both_step(n, _):
                @pl.when(n == dn_steps - 3)
                def _():
                    o_y.wait()
                    for c in o_hops:
                        c.start()
                slot = lax.rem(n, dn_slots)
                dn_copy(n, slot).wait()
                sent[0, n] = dot32(a[1], dnb[slot]).astype(BF16)
                sent[1, n] = dot32(a[0], dnb[slot]).astype(BF16)
                part_copy(0, n).start()

                @pl.when(n + dn_slots < dn_steps)
                def _():
                    dn_copy(n + dn_slots, slot).start()
                return 0
            lax.fori_loop(0, dn_steps, both_step, 0)
            for c in q_hops:
                c.wait()
            q_last.start()

            def fin(n, _):
                part_copy(0, n).wait()
                mix = (sent[1, n].astype(F32) + got[0, n].astype(F32)).astype(BF16)
                out_ref[:, cols_of(n)] = (h_ref[:, cols_of(n)].astype(F32) + mix.astype(F32)).astype(BF16)
                return 0
            lax.fori_loop(0, dn_steps, fin, 0)
            for c in o_hops:
                c.wait()
            o_last.start()
            for c in (t_last, q_last, o_last):
                c.wait()

    vmem = pl.BlockSpec(memory_space=pltpu.VMEM)
    sides = 1 if last else 2
    if last:
        outs = [jax.ShapeDtypeStruct((4, n, width), BF16) for n in splits]
        out_specs = [vmem, vmem]
    else:
        outs = [jax.ShapeDtypeStruct((rows, width), BF16), jax.ShapeDtypeStruct((4, width, hd), BF16), jax.ShapeDtypeStruct((4, hd, width), BF16)]
        out_specs = [vmem, ANY, ANY]
    nsem = 2 if last else 1
    scratch = ([] if last else [pltpu.VMEM((rows, width), BF16)]) + [
        pltpu.VMEM((rows, width), BF16), pltpu.VMEM((rows, width), BF16), pltpu.VMEM((sides, rows, ff), BF16),
        pltpu.VMEM((gu_slots, 2, width, bn), BF16), pltpu.VMEM((dn_slots, ff, dn), BF16),
        pltpu.VMEM((2, dn_steps, rows, dn), BF16), pltpu.VMEM((nsem, dn_steps, rows, dn), BF16),
        pltpu.SemaphoreType.DMA((gu_slots, 2)), pltpu.SemaphoreType.DMA((dn_slots,)), pltpu.SemaphoreType.DMA((2,)),
        pltpu.SemaphoreType.DMA((nsem, dn_steps)), pltpu.SemaphoreType.DMA((nsem, dn_steps)),
    ] + ([] if last else [pltpu.SemaphoreType.DMA((2, 11))])
    return pl.pallas_call(
        body, out_shape=outs, in_specs=[vmem] * (len(ins) + 1) + [ANY] * (5 if last else 6), out_specs=out_specs, scratch_shapes=scratch,
        compiler_params=pltpu.CompilerParams(vmem_limit_bytes=62 * MIB, collective_id=layer, has_side_effects=True), name=f"mlp{layer}",
        cost_estimate=cost(12 * rows * width * ff, 10 * width * ff),
    )(*ins, gain, w_gate, w_up, w_down, w_query, w_out, *([] if last else [wq_half]))


def after(value, *deps):
    return lax.optimization_barrier((value,) + deps)[0]


def solution(mesh):
    sp_size = mesh.shape["sp"]
    tp_size = mesh.shape["tp"]
    in_specs = (P("dp", "sp", None), P("dp", "sp"), P("dp"), P(), P(), P("tp", None), P(), P(None, None, "tp"), P(), P(), P(None, "tp", None), P(), P(None, None, "tp"), P(None, None, "tp"), P(None, "tp", None))
    out_specs = (P("dp", "sp", None), P("dp", "sp", None), P(None, None, "dp", "sp", None), P(None, None, "dp", "sp", None))
    swap = lambda v: lax.ppermute(v, "tp", [(i, tp_size - 1 - i) for i in range(tp_size)])

    def device_fn(features, tokens, lengths, proj_w, proj_b, embed, ln_attn, w_query, w_key, w_value, w_out, ln_mlp, w_gate, w_up, w_down):
        num_req, img_loc, _ = features.shape
        txt_loc = tokens.shape[1]
        seq = img_loc + txt_loc
        width = proj_w.shape[1]
        hd = w_key.shape[2]
        rows_loc = embed.shape[0]
        sp = lax.axis_index("sp")
        tp = lax.axis_index("tp")
        half = num_req // tp_size
        mine = lambda v, axis=0: lax.dynamic_slice_in_dim(v, tp * half, half, axis)
        theirs = lambda v, axis=0: lax.dynamic_slice_in_dim(v, (tp_size - 1 - tp) * half, half, axis)

        def rows_of(ids):
            return jnp.take(embed, jnp.clip(ids - tp * rows_loc, 0, rows_loc - 1), axis=0, mode="clip")

        def start_of(feats, ids, rows, got):
            owned = ((ids >= tp * rows_loc) & (ids < (tp + 1) * rows_loc)).astype(F32)
            img = (jnp.einsum("bpc,cd->bpd", feats, proj_w, preferred_element_type=F32) + proj_b.astype(F32)).astype(BF16)
            return (img, *rows, *got, owned[:, :, None])

        my_ids, their_ids = mine(tokens), theirs(tokens)
        picks, sent = [], []
        for ids in (my_ids[0], my_ids[1], their_ids[0], their_ids[1]):
            picks.append(rows_of(after(ids, *picks[-1:])))
            sent.append(swap(picks[-1]))

        positions = jnp.concatenate([sp * img_loc + jnp.arange(img_loc), img_loc * sp_size + sp * txt_loc + jnp.arange(txt_loc)])
        inv_freq = ROPE_THETA ** (-jnp.arange(hd // 2, dtype=F32) * (2.0 / hd))
        angles = positions.astype(F32)[:, None] * inv_freq[None, :]
        cos, sin = jnp.cos(angles), jnp.sin(angles)
        slot = jnp.arange(seq)[None, :]
        owner = jnp.stack([sp ^ b for b in range(sp_size)])[:, None]
        text_index = (owner * txt_loc + slot - img_loc).reshape(1, -1)
        is_img = jnp.broadcast_to(slot < img_loc, (sp_size, seq)).reshape(1, -1)
        mask_of = lambda lens: (is_img | (text_index < lens[:, None])).astype(F32)[:, None, :]
        my_mask, their_mask = mask_of(mine(lengths)), mask_of(theirs(lengths))

        weights = (w_key, w_value, w_query, w_out)
        their_h = start_of(theirs(features), their_ids, picks[2:], sent[:2])
        their_kv, their_part, wq_half = attention(0, their_h, ln_attn, *weights, None, cos, sin, their_mask, "t", 2, ahead=True)
        back = swap(their_part)
        my_h = start_of(mine(features), my_ids, picks[:2], sent[2:])
        kv, part, hidden = attention(0, my_h, ln_attn, *weights, None, cos, sin, my_mask, "m", 3, keep=True)
        pair = [v.reshape(2, half, seq, hd) for v in (kv, their_kv)]
        caches = [jnp.where(tp == 0, jnp.concatenate(pair, axis=1), jnp.concatenate(pair[::-1], axis=1))]
        hidden, wq_next, wo_next = mlp(0, (hidden, part, back), ln_mlp, w_gate, w_up, w_down, w_query, w_out, wq_half)

        kv, h1 = attention(1, hidden, ln_attn, *weights, (wq_next, wo_next, wq_half), cos, sin, my_mask, "m", 4)
        caches.append(kv.reshape(2, num_req, seq, hd))
        final = mlp(1, h1, ln_mlp, w_gate, w_up, w_down, w_query, w_out, splits=(img_loc, txt_loc))

        cache = jnp.stack(caches)
        return final[0], final[1], cache[:, :, :, :img_loc], cache[:, :, :, img_loc:]

    return jax.shard_map(device_fn, mesh=mesh, in_specs=in_specs, out_specs=out_specs, check_vma=False)
```
